8 devices in a mesh: dp: 2 (over z, y), ep: 4 (over x, core).
Axes of the slice: x: 2, y: 2, z: 1, core: 2. Of those that a mesh axis runs over, the one named last changes fastest.
Arguments:
- tokens: bfloat16 [8, 512, 2048], P(('dp', 'ep')), parts along dimension 0
- w_query: bfloat16 [2048, 16, 128], P('ep')
- w_key: bfloat16 [2048, 16, 128], P('ep')
- w_value: bfloat16 [2048, 16, 128], P('ep')
- w_out: bfloat16 [2048, 2048], P('ep')
- w_router: float32 [2048, 64], replicated
- w_one: bfloat16 [64, 2048, 1024], P('ep')
- w_three: bfloat16 [64, 2048, 1024], P('ep')
- w_two: bfloat16 [64, 1024, 2048], P('ep')
- expert_ids: int32 [8, 512, 8], P(('dp', 'ep')), parts along dimension 0
Outputs:
- output: bfloat16 [8, 512, 2048], P(('dp', 'ep')), parts along dimension 0
There are 2 independent parts. The reference program is written for one: setup_inputs(seed, part) draws one part's arguments, and reference() takes and returns one part's arrays. A program takes and returns all parts, laid end to end along the dimension named above; an argument that names none is the same for every part.
All inputs are finite; a program needn't handle non-finite values.
Results may differ from the reference program's by a relative error of at most 0.00977733.
Values are sent between devices in bfloat16 or wider.
A program may use at most 1 GiB of HBM per device.

```python
import jax
import jax.numpy as jnp
import numpy as np
from jax import lax

D = 2048
HEADS = 16
HEAD = 128
EXPERTS = 64
TOP = 8
FF = 1024
TOK_DEV = 512
SEQ = 512
GROUP = 4

TOKENS = TOK_DEV * GROUP
N_SEQ = TOKENS // SEQ
CAP = 2 * TOK_DEV * TOP // EXPERTS
WIDTH = HEADS * HEAD
EPS = 1e-6


def draw_routing(route_key):
    mean_load = TOK_DEV * TOP // EXPERTS
    ranks = np.arange(EXPERTS)
    loads = np.where(ranks < EXPERTS // 4, 2 * mean_load, np.where(ranks < EXPERTS // 2, mean_load, mean_load // 2))
    rank_of_pos = np.repeat(ranks, loads)
    order_key, device_key = jax.random.split(route_key)
    expert_order = jax.random.permutation(order_key, EXPERTS)
    grid = expert_order[rank_of_pos].reshape(TOP, TOK_DEV).T

    def one_device(dev_key):
        perm_key, shift_key = jax.random.split(dev_key)
        token_order = jax.random.permutation(perm_key, TOK_DEV)
        shift = jax.random.randint(shift_key, (TOK_DEV, 1), 0, TOP)
        columns = (jnp.arange(TOP)[None, :] + shift) % TOP
        return jnp.take_along_axis(grid[token_order], columns, axis=1)

    routes = jax.vmap(one_device)(jax.random.split(device_key, GROUP))
    return routes.reshape(N_SEQ, SEQ, TOP).astype(jnp.int32)


def setup_inputs(seed: int = 0, part: int = 0) -> dict:
    root_key = jax.random.key(seed)
    part_keys = jax.random.split(jax.random.fold_in(root_key, part), 3)
    weight_keys = jax.random.split(root_key, 8)

    def gaussian(index, shape, scale):
        return scale * jax.random.normal(weight_keys[index], shape, jnp.float32)

    seq_base = jax.random.normal(part_keys[0], (N_SEQ, 1, D), jnp.float32)
    noise = jax.random.normal(part_keys[1], (N_SEQ, SEQ, D), jnp.float32)
    return {
        'tokens': (0.6 * seq_base + 0.8 * noise).astype(jnp.bfloat16),
        'w_query': gaussian(0, (D, HEADS, HEAD), 1.5 * D ** -0.5).astype(jnp.bfloat16),
        'w_key': gaussian(1, (D, HEADS, HEAD), 1.5 * D ** -0.5).astype(jnp.bfloat16),
        'w_value': gaussian(2, (D, HEADS, HEAD), D ** -0.5).astype(jnp.bfloat16),
        'w_out': gaussian(3, (WIDTH, D), WIDTH ** -0.5).astype(jnp.bfloat16),
        'w_router': gaussian(4, (D, EXPERTS), D ** -0.5),
        'w_one': gaussian(5, (EXPERTS, D, FF), D ** -0.5).astype(jnp.bfloat16),
        'w_three': gaussian(6, (EXPERTS, D, FF), D ** -0.5).astype(jnp.bfloat16),
        'w_two': gaussian(7, (EXPERTS, FF, D), 2.0 * FF ** -0.5).astype(jnp.bfloat16),
        'expert_ids': draw_routing(part_keys[2]),
    }


def rms_norm(vals):
    wide = vals.astype(jnp.float32)
    return wide * lax.rsqrt(jnp.mean(wide * wide, axis=-1, keepdims=True) + EPS)


def reference(tokens, w_query, w_key, w_value, w_out, w_router, w_one, w_three, w_two, expert_ids):
    flat_query = w_query.reshape(D, WIDTH)
    flat_key = w_key.reshape(D, WIDTH)
    flat_value = w_value.reshape(D, WIDTH)
    causal = jnp.arange(SEQ)[:, None] >= jnp.arange(SEQ)[None, :]

    def one_sequence(seq_tokens):
        normed = rms_norm(seq_tokens).astype(jnp.bfloat16)
        query = jnp.dot(normed, flat_query, preferred_element_type=jnp.float32).astype(jnp.bfloat16)
        keys = jnp.dot(normed, flat_key, preferred_element_type=jnp.float32).astype(jnp.bfloat16)
        values = jnp.dot(normed, flat_value, preferred_element_type=jnp.float32).astype(jnp.bfloat16)
        query = query.astype(jnp.float32).reshape(SEQ, HEADS, HEAD)
        keys = keys.astype(jnp.float32).reshape(SEQ, HEADS, HEAD)
        values = values.astype(jnp.float32).reshape(SEQ, HEADS, HEAD)
        scores = jnp.einsum('qhk,shk->hqs', query, keys) * HEAD ** -0.5
        scores = jnp.where(causal, scores, -jnp.inf)
        attn_weights = jax.nn.softmax(scores, axis=-1).astype(jnp.bfloat16).astype(jnp.float32)
        context = jnp.einsum('hqs,shk->qhk', attn_weights, values).astype(jnp.bfloat16)
        attn_out = jnp.dot(context.reshape(SEQ, WIDTH), w_out, preferred_element_type=jnp.float32)
        return (seq_tokens.astype(jnp.float32) + attn_out).astype(jnp.bfloat16)

    hidden = lax.map(one_sequence, tokens).reshape(TOKENS, D)
    normed = rms_norm(hidden)
    logits = jnp.dot(normed, w_router, preferred_element_type=jnp.float32)
    ids_flat = expert_ids.reshape(TOKENS, TOP)
    gates = jax.nn.softmax(jnp.take_along_axis(logits, ids_flat, axis=1), axis=-1)
    padded = jnp.concatenate([normed.astype(jnp.bfloat16), jnp.zeros((1, D), jnp.bfloat16)], axis=0)
    limit = GROUP * CAP

    def one_expert(total_mix, expert_pack):
        expert, first_w, third_w, second_w = expert_pack
        match = ids_flat == expert
        weight = jnp.sum(jnp.where(match, gates, 0.0), axis=1)
        rows = jnp.nonzero(jnp.any(match, axis=1), size=limit, fill_value=TOKENS)[0]
        picked = padded[rows]
        first = jnp.dot(picked, first_w, preferred_element_type=jnp.float32)
        third = jnp.dot(picked, third_w, preferred_element_type=jnp.float32)
        activated = (jax.nn.silu(first) * third).astype(jnp.bfloat16)
        result = jnp.dot(activated, second_w, preferred_element_type=jnp.float32).astype(jnp.bfloat16)
        scale = jnp.concatenate([weight, jnp.zeros((1,), jnp.float32)])[rows]
        total_mix = total_mix.at[rows].add(scale[:, None] * result.astype(jnp.float32), mode='drop')
        return total_mix, None

    total_mix, _ = lax.scan(one_expert, jnp.zeros((TOKENS, D), jnp.float32), (jnp.arange(EXPERTS), w_one, w_three, w_two))
    layer_out = (hidden.astype(jnp.float32) + total_mix).astype(jnp.bfloat16)
    return layer_out.reshape(N_SEQ, SEQ, D)
```

```python
import functools
import jax
import jax.numpy as jnp
from jax import lax
from jax.experimental import pallas as pl
from jax.experimental.pallas import tpu as pltpu
from jax.sharding import PartitionSpec as P

EPS = 1e-6
PAIR = [(0, 1), (1, 0), (2, 3), (3, 2)]
ACROSS = [(0, 2), (2, 0), (1, 3), (3, 1)]
SWAP = [(0, 1), (1, 0)]
VMEM_CAP = 60 * 1024 * 1024
F32 = jnp.float32
BF16 = jnp.bfloat16


def rms_norm(vals):
    wide = vals.astype(F32)
    return wide * lax.rsqrt(jnp.mean(wide * wide, axis=-1, keepdims=True) + EPS)


def params(*semantics):
    return pltpu.CompilerParams(dimension_semantics=semantics, vmem_limit_bytes=VMEM_CAP)


def piece_sum(offs_ref, left_ref, piece_refs):
    total = None
    for idx, ref in enumerate(piece_refs):
        depth = ref.shape[0]
        cols = pl.ds(pl.multiple_of(offs_ref[idx], depth), depth)
        part = jnp.dot(left_ref[:, cols], ref[...], preferred_element_type=F32)
        total = part if total is None else total + part
    return total


def proj_kernel(offs_ref, left_ref, *refs):
    refs[-1][...] = piece_sum(offs_ref, left_ref, refs[:-1]).astype(BF16)


def project(offs, normed, pieces, block=512):
    rows, depth = normed.shape
    cols = pieces[0].shape[1]
    specs = [pl.BlockSpec((piece.shape[0], block), lambda n: (0, n)) for piece in pieces]
    return pl.pallas_call(
        proj_kernel,
        grid=(cols // block,),
        in_specs=[pl.BlockSpec(memory_space=pltpu.SMEM), pl.BlockSpec((rows, depth), lambda n: (0, 0))] + specs,
        out_specs=pl.BlockSpec((rows, block), lambda n: (0, n)),
        out_shape=jax.ShapeDtypeStruct((rows, cols), BF16),
        compiler_params=params('arbitrary'),
        cost_estimate=pl.CostEstimate(flops=2 * rows * depth * cols, bytes_accessed=2 * depth * cols, transcendentals=0),
        name='project',
    )(offs, normed, *pieces)


def attn_kernel(q_ref, k_ref, v_ref, o_ref, *, rows, scale):
    seq = q_ref.shape[0]
    for head in range(q_ref.shape[1] // 128):
        lanes = slice(head * 128, head * 128 + 128)
        for start in range(0, seq, rows):
            stop = start + rows
            scores = lax.dot_general(q_ref[start:stop, lanes], k_ref[:stop, lanes], (((1,), (1,)), ((), ())),
                                     preferred_element_type=F32) * scale
            row_id = lax.broadcasted_iota(jnp.int32, (rows, stop), 0) + start
            col_id = lax.broadcasted_iota(jnp.int32, (rows, stop), 1)
            scores = jnp.where(row_id >= col_id, scores, -jnp.inf)
            top = jnp.max(scores, axis=-1, keepdims=True)
            expo = jnp.exp(scores - top)
            weights = (expo / jnp.sum(expo, axis=-1, keepdims=True)).astype(BF16)
            o_ref[start:stop, lanes] = jnp.dot(weights, v_ref[:stop, lanes], preferred_element_type=F32).astype(BF16)


def attend(query, keys, values, head_dim, heads_step=2):
    seq, width = query.shape
    block = head_dim * heads_step
    spec = pl.BlockSpec((seq, block), lambda h: (0, h))
    return pl.pallas_call(
        functools.partial(attn_kernel, rows=128, scale=head_dim ** -0.5),
        grid=(width // block,),
        in_specs=[spec] * 3,
        out_specs=spec,
        out_shape=jax.ShapeDtypeStruct((seq, width), BF16),
        compiler_params=params('arbitrary'),
        cost_estimate=pl.CostEstimate(flops=8 * seq * seq * width, bytes_accessed=8 * seq * width, transcendentals=0),
        name='attend',
    )(query, keys, values)


def out_kernel(offs_ref, left_ref, x_ref, *refs):
    hidden = (x_ref[...].astype(F32) + piece_sum(offs_ref, left_ref, refs[:-2])).astype(BF16)
    refs[-2][...] = hidden
    refs[-1][...] = rms_norm(hidden).astype(BF16)


def out_project(offs, context, tokens, pieces, block=256):
    rows, depth = context.shape
    cols = pieces[0].shape[1]
    row_spec = pl.BlockSpec((block, cols), lambda m: (m, 0))
    return pl.pallas_call(
        out_kernel,
        grid=(rows // block,),
        in_specs=[pl.BlockSpec(memory_space=pltpu.SMEM), pl.BlockSpec((block, depth), lambda m: (m, 0)), row_spec]
        + [pl.BlockSpec(piece.shape, lambda m: (0, 0)) for piece in pieces],
        out_specs=[row_spec, row_spec],
        out_shape=[jax.ShapeDtypeStruct((rows, cols), BF16)] * 2,
        compiler_params=params('arbitrary'),
        cost_estimate=pl.CostEstimate(flops=2 * rows * depth * cols, bytes_accessed=2 * depth * cols, transcendentals=0),
        name='out_project',
    )(offs, context, tokens, *pieces)


def up_kernel(pos_lane_ref, pos_ref, gate_ref, u0_ref, u1_ref, w1_ref, w3_ref, act_ref, mix_ref, rows_ref, *, cap):
    expert = pl.program_id(0)
    seq = u0_ref.shape[0]
    slots = lax.broadcasted_iota(jnp.int32, (cap, seq), 0)
    for src, u_ref in enumerate((u0_ref, u1_ref)):
        pick = (pos_lane_ref[0, src:src + 1, :] == slots).astype(F32).astype(BF16)
        rows_ref[src * cap:(src + 1) * cap, :] = jnp.dot(pick, u_ref[...], preferred_element_type=F32).astype(BF16)
    rows = rows_ref[...]
    first = jnp.dot(rows, w1_ref[0], preferred_element_type=F32)
    third = jnp.dot(rows, w3_ref[0], preferred_element_type=F32)
    act_ref[0] = (jax.nn.silu(first) * third).astype(BF16)
    lanes = lax.broadcasted_iota(jnp.int32, (seq, pos_ref.shape[2]), 1)
    cap_lanes = lax.broadcasted_iota(jnp.int32, (seq, cap), 1)
    for src in range(2):
        place = jnp.sum(jnp.where(lanes == expert, pos_ref[src], 0), axis=-1, keepdims=True)
        gate = jnp.sum(jnp.where(lanes == expert, gate_ref[src], 0.0), axis=-1, keepdims=True)
        hit = place == cap_lanes
        rest = gate
        for term in range(3):
            part = rest.astype(BF16).astype(F32)
            mix_ref[src, :, term * cap:(term + 1) * cap] = jnp.where(hit, part, 0.0).astype(BF16)
            rest = rest - part


def expert_up(pos_lane, pos, gates, u0, u1, w_one, w_three, cap):
    count, depth, width = w_one.shape
    seq = u0.shape[0]
    whole2 = pl.BlockSpec((seq, depth), lambda e: (0, 0))
    whole3 = pl.BlockSpec((2, seq, count), lambda e: (0, 0, 0))
    w_spec = pl.BlockSpec((1, depth, width), lambda e: (e, 0, 0))
    return pl.pallas_call(
        functools.partial(up_kernel, cap=cap),
        grid=(count,),
        in_specs=[pl.BlockSpec((1, 2, seq), lambda e: (e, 0, 0)), whole3, whole3, whole2, whole2, w_spec, w_spec],
        out_specs=[pl.BlockSpec((1, 2 * cap, width), lambda e: (e, 0, 0)),
                   pl.BlockSpec((2, seq, 3 * cap), lambda e: (0, 0, e))],
        out_shape=[jax.ShapeDtypeStruct((count, 2 * cap, width), BF16),
                   jax.ShapeDtypeStruct((2, seq, count * 3 * cap), BF16)],
        scratch_shapes=[pltpu.VMEM((2 * cap, depth), BF16)],
        compiler_params=params('arbitrary'),
        cost_estimate=pl.CostEstimate(flops=8 * cap * depth * width * count + 4 * cap * seq * depth * count,
                                      bytes_accessed=4 * count * depth * width, transcendentals=0),
        name='expert_up',
    )(pos_lane, pos, gates, u0, u1, w_one, w_three)


def down_kernel(act_ref, w2_ref, mix_ref, out_ref, *, cap, per):
    @pl.when(pl.program_id(0) == 0)
    def _():
        out_ref[...] = jnp.zeros_like(out_ref)

    stack = [[], []]
    for idx in range(per):
        done = jnp.dot(act_ref[idx], w2_ref[idx], preferred_element_type=F32).astype(BF16)
        for src in range(2):
            stack[src] += [done[src * cap:(src + 1) * cap]] * 3
    for src in range(2):
        out_ref[src] += jnp.dot(mix_ref[src], jnp.concatenate(stack[src], axis=0), preferred_element_type=F32)


def expert_down(act, w_two, mix, cap, part, parts, per=2):
    count, width, model = w_two.shape
    seq = mix.shape[1]
    block = model // parts
    return pl.pallas_call(
        functools.partial(down_kernel, cap=cap, per=per),
        grid=(count // per,),
        in_specs=[pl.BlockSpec((per, 2 * cap, width), lambda e: (e, 0, 0)),
                  pl.BlockSpec((per, width, block), lambda e: (e, 0, part)),
                  pl.BlockSpec((2, seq, 3 * cap * per), lambda e: (0, 0, e))],
        out_specs=pl.BlockSpec((2, seq, block), lambda e: (0, 0, 0)),
        out_shape=jax.ShapeDtypeStruct((2, seq, block), F32),
        compiler_params=params('arbitrary'),
        cost_estimate=pl.CostEstimate(flops=(4 * cap * width * block + 12 * seq * cap * block) * count,
                                      bytes_accessed=2 * count * width * block, transcendentals=0),
        name='expert_down',
    )(act, w_two, mix)


def solution(mesh):
    tok_spec = P(('dp', 'ep'))
    row_spec = P('ep')

    def local_layer(tokens, w_query, w_key, w_value, w_out, w_router, w_one, w_three, w_two, expert_ids):
        seq, model = tokens.shape[1:]
        head_dim = w_query.shape[2]
        choices = expert_ids.shape[2]
        experts = w_router.shape[1]
        own_experts = w_one.shape[0]
        cap = 2 * seq * choices // experts
        group = lax.axis_index('dp')
        me = lax.axis_index('ep')
        x_rows = tokens[0]
        shard = w_out.shape[0]
        half = shard // 2

        pair = functools.partial(lax.ppermute, axis_name='ep', perm=PAIR)
        across = functools.partial(lax.ppermute, axis_name='ep', perm=ACROSS)
        swap = functools.partial(lax.ppermute, axis_name='dp', perm=SWAP)

        def gather(weight):
            mine = lax.dynamic_slice_in_dim(weight, group * half, half, 0).reshape(half, -1)
            full = weight.reshape(shard, -1)
            far = across(mine)
            far_other = swap(far)
            return [full, pair(full), far, far_other, pair(far), pair(far_other)]

        offs = jnp.stack([me * shard, (me ^ 1) * shard,
                          (me ^ 2) * shard + group * half, (me ^ 2) * shard + (1 - group) * half,
                          (me ^ 3) * shard + group * half, (me ^ 3) * shard + (1 - group) * half]).astype(jnp.int32)
        q_parts, k_parts, v_parts, o_parts = [gather(w) for w in (w_query, w_key, w_value, w_out)]

        ids = expert_ids[0]
        ids_pair = pair(ids)
        ids_far = across(ids)
        ids_all = jnp.stack([ids, ids_pair, ids_far, pair(ids_far)])
        mine = me * own_experts + jnp.arange(own_experts, dtype=jnp.int32)
        member = jnp.any(ids_all[:, :, :, None] == mine, axis=2)
        count = member.astype(jnp.int32)
        pos = jnp.where(member, jnp.cumsum(count, axis=1) - count, -1)
        pos_lane = pos.transpose(2, 0, 1)

        normed = rms_norm(x_rows).astype(BF16)
        query = project(offs, normed, q_parts)
        keys = project(offs, normed, k_parts)
        values = project(offs, normed, v_parts)
        context = attend(query, keys, values, head_dim)
        hidden, u_own = out_project(offs, context, x_rows, o_parts)

        u_far = across(u_own)
        u_pair = pair(u_own)
        u_far_pair = pair(u_far)

        logits = jnp.dot(rms_norm(hidden), w_router, precision=lax.Precision.HIGHEST, preferred_element_type=F32)
        chosen = jnp.any(ids[:, :, None] == jnp.arange(experts, dtype=jnp.int32), axis=1)
        gates = jax.nn.softmax(jnp.where(chosen, logits, -jnp.inf), axis=-1)
        gates_far = across(gates)
        pick = functools.partial(lax.dynamic_slice_in_dim, start_index=me * own_experts, slice_size=own_experts, axis=1)
        gates_near = jnp.stack([pick(gates), pick(pair(gates))])
        gates_away = jnp.stack([pick(gates_far), pick(pair(gates_far))])

        act_near, mix_near = expert_up(pos_lane[:, 0:2], pos[0:2], gates_near, u_own, u_pair, w_one, w_three, cap)
        act_away, mix_away = expert_up(pos_lane[:, 2:4], pos[2:4], gates_away, u_far, u_far_pair, w_one, w_three, cap)

        parts = 4
        back = []
        for part in range(parts):
            sums = expert_down(act_away, w_two, mix_away, cap, part, parts)
            back.append(across(sums[0] + pair(sums[1])))
        outs = []
        for part in range(parts):
            sums = expert_down(act_near, w_two, mix_near, cap, part, parts)
            block = model // parts
            near = hidden[:, part * block:(part + 1) * block].astype(F32) + (sums[0] + pair(sums[1]))
            outs.append((near + back[part]).astype(BF16))
        return jnp.concatenate(outs, axis=1)[None]

    return jax.shard_map(local_layer, mesh=mesh, in_specs=(tok_spec, row_spec, row_spec, row_spec, row_spec, P(), row_spec, row_spec, row_spec, tok_spec), out_specs=tok_spec, check_vma=False)
```

```python
import functools
import jax
import jax.numpy as jnp
from jax import lax
from jax.experimental import pallas as pl
from jax.experimental.pallas import tpu as pltpu
from jax.sharding import PartitionSpec as P

EPS = 1e-6
PAIR = [(0, 1), (1, 0), (2, 3), (3, 2)]
ACROSS = [(0, 2), (2, 0), (1, 3), (3, 1)]
SWAP = [(0, 1), (1, 0)]
VMEM_CAP = 60 * 1024 * 1024
F32 = jnp.float32
BF16 = jnp.bfloat16


def rms_norm(vals):
    wide = vals.astype(F32)
    return wide * lax.rsqrt(jnp.mean(wide * wide, axis=-1, keepdims=True) + EPS)


def params(*semantics):
    return pltpu.CompilerParams(dimension_semantics=semantics, vmem_limit_bytes=VMEM_CAP)


def piece_sum(offs_ref, left_ref, piece_refs):
    total = None
    for idx, ref in enumerate(piece_refs):
        depth = ref.shape[0]
        cols = pl.ds(pl.multiple_of(offs_ref[idx], depth), depth)
        part = jnp.dot(left_ref[:, cols], ref[...], preferred_element_type=F32)
        total = part if total is None else total + part
    return total


def proj_kernel(offs_ref, left_ref, *refs):
    refs[-1][...] = piece_sum(offs_ref, left_ref, refs[:-1]).astype(BF16)


def project(offs, normed, pieces, block=512):
    rows, depth = normed.shape
    cols = pieces[0].shape[1]
    specs = [pl.BlockSpec((piece.shape[0], block), lambda n: (0, n)) for piece in pieces]
    return pl.pallas_call(
        proj_kernel,
        grid=(cols // block,),
        in_specs=[pl.BlockSpec(memory_space=pltpu.SMEM), pl.BlockSpec((rows, depth), lambda n: (0, 0))] + specs,
        out_specs=pl.BlockSpec((rows, block), lambda n: (0, n)),
        out_shape=jax.ShapeDtypeStruct((rows, cols), BF16),
        compiler_params=params('arbitrary'),
        cost_estimate=pl.CostEstimate(flops=2 * rows * depth * cols, bytes_accessed=2 * depth * cols, transcendentals=0),
        name='project',
    )(offs, normed, *pieces)


def attn_kernel(q_ref, k_ref, v_ref, o_ref, *, rows, scale):
    seq = q_ref.shape[0]
    for head in range(q_ref.shape[1] // 128):
        lanes = slice(head * 128, head * 128 + 128)
        for start in range(0, seq, rows):
            stop = start + rows
            scores = lax.dot_general(q_ref[start:stop, lanes], k_ref[:stop, lanes], (((1,), (1,)), ((), ())),
                                     preferred_element_type=F32) * scale
            row_id = lax.broadcasted_iota(jnp.int32, (rows, stop), 0) + start
            col_id = lax.broadcasted_iota(jnp.int32, (rows, stop), 1)
            scores = jnp.where(row_id >= col_id, scores, -jnp.inf)
            top = jnp.max(scores, axis=-1, keepdims=True)
            expo = jnp.exp(scores - top)
            weights = (expo / jnp.sum(expo, axis=-1, keepdims=True)).astype(BF16)
            o_ref[start:stop, lanes] = jnp.dot(weights, v_ref[:stop, lanes], preferred_element_type=F32).astype(BF16)


def attend(query, keys, values, head_dim, heads_step=2):
    seq, width = query.shape
    block = head_dim * heads_step
    spec = pl.BlockSpec((seq, block), lambda h: (0, h))
    return pl.pallas_call(
        functools.partial(attn_kernel, rows=128, scale=head_dim ** -0.5),
        grid=(width // block,),
        in_specs=[spec] * 3,
        out_specs=spec,
        out_shape=jax.ShapeDtypeStruct((seq, width), BF16),
        compiler_params=params('arbitrary'),
        cost_estimate=pl.CostEstimate(flops=8 * seq * seq * width, bytes_accessed=8 * seq * width, transcendentals=0),
        name='attend',
    )(query, keys, values)


def out_kernel(offs_ref, left_ref, x_ref, *refs):
    hidden = (x_ref[...].astype(F32) + piece_sum(offs_ref, left_ref, refs[:-2])).astype(BF16)
    refs[-2][...] = hidden
    refs[-1][...] = rms_norm(hidden).astype(BF16)


def out_project(offs, context, tokens, pieces, block=256):
    rows, depth = context.shape
    cols = pieces[0].shape[1]
    row_spec = pl.BlockSpec((block, cols), lambda m: (m, 0))
    return pl.pallas_call(
        out_kernel,
        grid=(rows // block,),
        in_specs=[pl.BlockSpec(memory_space=pltpu.SMEM), pl.BlockSpec((block, depth), lambda m: (m, 0)), row_spec]
        + [pl.BlockSpec(piece.shape, lambda m: (0, 0)) for piece in pieces],
        out_specs=[row_spec, row_spec],
        out_shape=[jax.ShapeDtypeStruct((rows, cols), BF16)] * 2,
        compiler_params=params('arbitrary'),
        cost_estimate=pl.CostEstimate(flops=2 * rows * depth * cols, bytes_accessed=2 * depth * cols, transcendentals=0),
        name='out_project',
    )(offs, context, tokens, *pieces)


def spread_kernel(pos_ref, out_ref):
    expert = pl.program_id(1)
    seq = pos_ref.shape[1]
    lanes = lax.broadcasted_iota(jnp.int32, (seq, pos_ref.shape[2]), 1)
    place = jnp.sum(jnp.where(lanes == expert, pos_ref[0], 0), axis=-1, keepdims=True)
    slots = lax.broadcasted_iota(jnp.int32, (seq, out_ref.shape[2]), 1)
    out_ref[0] = (place == slots).astype(F32).astype(BF16)


def spread(pos, cap):
    sources, seq, count = pos.shape
    return pl.pallas_call(
        spread_kernel,
        grid=(sources, count),
        in_specs=[pl.BlockSpec((1, seq, count), lambda s, e: (s, 0, 0))],
        out_specs=pl.BlockSpec((1, seq, cap), lambda s, e: (s, 0, e)),
        out_shape=jax.ShapeDtypeStruct((sources, seq, count * cap), BF16),
        compiler_params=params('arbitrary', 'arbitrary'),
        name='spread',
    )(pos)


def moe_kernel(pos_ref, u_ref, gate_ref, hid_ref, w1_ref, w3_ref, w2_ref, oh_ref, out_ref,
               ug, gg, rows, act, gcol, w13, w2t, oht, pst, acc, pair_buf, far_src, far_dst,
               us, ur, gs, gr, ws, w2s, ohs, ps, pr, xs, xr,
               *, cap, u_chunks, chunks, groups, wslots):
    me = lax.axis_index('ep')
    relations = (me ^ 1, me ^ 2, me ^ 3)
    seq, model = u_ref.shape
    count, _, width = w1_ref.shape
    col = width // wslots
    block = model // chunks
    per = count // groups
    piece = seq // u_chunks

    def remote(src, dst, send, recv, relation):
        return pltpu.make_async_remote_copy(src_ref=src, dst_ref=dst, send_sem=send, recv_sem=recv,
                                            device_id={'ep': relations[relation]}, device_id_type=pl.DeviceIdType.MESH)

    def w13_copy(expert, slot, which):
        ref = (w1_ref, w3_ref)[which]
        return pltpu.make_async_copy(ref.at[expert, :, pl.ds(slot * col, col)], w13.at[slot, which], ws.at[slot, which])

    def w2_copy(chunk, part, slot):
        return pltpu.make_async_copy(w2_ref.at[pl.ds(part * per, per), :, pl.ds(pl.multiple_of(chunk * block, block), block)],
                                     w2t.at[slot], w2s.at[slot])

    def oh_copy(phase, part, slot):
        return pltpu.make_async_copy(oh_ref.at[pl.ds(2 * phase, 2), :, pl.ds(part * per * cap, per * cap)],
                                     oht.at[slot], ohs.at[slot])

    for slot in range(wslots):
        w13_copy(0, slot, 0).start()
        w13_copy(0, slot, 1).start()

    barrier = pltpu.get_barrier_semaphore()
    for peer in relations:
        pl.semaphore_signal(barrier, inc=1, device_id={'ep': peer}, device_id_type=pl.DeviceIdType.MESH)
    pl.semaphore_wait(barrier, 3)

    gate_sends = [remote(gate_ref.at[pl.ds(pl.multiple_of(relations[r] * count, count), count)], gg.at[r], gs.at[r], gr.at[r], r)
                  for r in range(3)]
    pair_send = remote(u_ref, ug.at[0], us.at[0], ur.at[0], 0)

    def far_send(idx):
        part = pl.ds(idx * piece, piece)
        return remote(u_ref.at[part], ug.at[1, part], us.at[1 + idx], ur.at[1 + idx], 1)

    def relay_send(idx):
        part = pl.ds(idx * piece, piece)
        return remote(ug.at[1, part], ug.at[2, part], us.at[1 + u_chunks + idx], ur.at[1 + u_chunks + idx], 0)

    for send in gate_sends:
        send.start()
    for idx in range(u_chunks):
        far_send(idx).start()
    pair_send.start()

    slots = lax.broadcasted_iota(jnp.int32, (cap, seq), 0)
    lanes = lax.broadcasted_iota(jnp.int32, (2 * cap, 128), 1)

    def up_step(phase, expert):
        place = pos_ref[expert]
        if phase == 0:
            sources = ((u_ref[...], gate_ref[pl.ds(me * count + expert, 1), :]), (ug[0], gg[0, pl.ds(expert, 1), :]))
        else:
            sources = ((ug[1], gg[1, pl.ds(expert, 1), :]), (ug[2], gg[2, pl.ds(expert, 1), :]))
        for src, (u_val, gate_row) in enumerate(sources):
            hit = place[2 * phase + src:2 * phase + src + 1, :] == slots
            rows[src * cap:(src + 1) * cap, :] = jnp.dot(hit.astype(F32).astype(BF16), u_val,
                                                         preferred_element_type=F32).astype(BF16)
            column = jnp.sum(jnp.where(hit, gate_row, 0.0), axis=-1, keepdims=True)
            part = slice(src * cap, (src + 1) * cap)
            gcol[phase, part, :] = jnp.where(lanes[part] == expert, column, gcol[phase, part, :])
        for slot in range(wslots):
            w13_copy(0, slot, 0).wait()
            w13_copy(0, slot, 1).wait()
            first = jnp.dot(rows[...], w13[slot, 0], preferred_element_type=F32)
            third = jnp.dot(rows[...], w13[slot, 1], preferred_element_type=F32)
            act[phase * count + expert, :, slot * col:(slot + 1) * col] = (jax.nn.silu(first) * third).astype(BF16)

            def refill(slot=slot):
                following = lax.rem(expert + 1, count)
                w13_copy(following, slot, 0).start()
                w13_copy(following, slot, 1).start()

            if phase == 0:
                refill()
            else:
                pl.when(expert < count - 1)(refill)

    gcol[...] = jnp.zeros_like(gcol)
    gate_sends[0].wait_recv()
    pair_send.wait_recv()
    step = count // u_chunks
    for idx in range(u_chunks):
        def near(expert, carry):
            up_step(0, expert)
            return carry
        lax.fori_loop(idx * step, (idx + 1) * step, near, 0)
        far_send(idx).wait_recv()
        relay_send(idx).start()
    for idx in range(3):
        w2_copy(0, idx, idx).start()
        oh_copy(1, idx, idx).start()
    gate_sends[1].wait_recv()
    gate_sends[2].wait_recv()
    for idx in range(u_chunks):
        relay_send(idx).wait_recv()

    def away(expert, carry):
        up_step(1, expert)
        return carry
    lax.fori_loop(0, count, away, 0)

    def down_chunk(phase, chunk):
        order = (1 - phase) * chunks + chunk
        for part in range(groups):
            slot = lax.rem(order * groups + part, 3)
            w2_copy(0, 0, slot).wait()
            oh_copy(0, 0, slot).wait()
            for idx in range(per):
                expert = part * per + idx
                done = jnp.dot(act[phase * count + expert], w2t[slot, idx], preferred_element_type=F32).astype(BF16)
                rest = done.astype(F32) * gcol[phase, :, expert:expert + 1]
                for term in range(3):
                    head = rest.astype(BF16)
                    at = (term * per + idx) * cap
                    pst[0, at:at + cap, :] = head[:cap]
                    pst[1, at:at + cap, :] = head[cap:]
                    rest = rest - head.astype(F32)
            depth = per * cap
            for src in range(2):
                mixed = jnp.dot(oht[slot, src], pst[src, 0:depth, :], preferred_element_type=F32)
                for term in range(1, 3):
                    mixed += jnp.dot(oht[slot, src], pst[src, term * depth:(term + 1) * depth, :], preferred_element_type=F32)
                if part == 0:
                    acc[lax.rem(chunk, 2), src] = mixed
                else:
                    acc[lax.rem(chunk, 2), src] += mixed

            def refill(part=part, slot=slot):
                ahead = order * groups + part + 3
                ahead_chunk = lax.rem(ahead // groups, chunks)
                ahead_part = lax.rem(ahead, groups)
                ahead_phase = 1 - ahead // (groups * chunks)
                w2_copy(ahead_chunk, ahead_part, slot).start()
                oh_copy(ahead_phase, ahead_part, slot).start()

            if phase == 1:
                refill()
            else:
                pl.when(order * groups + part + 3 < 2 * groups * chunks)(refill)

    def pair_sum(phase, chunk):
        slot = lax.rem((1 - phase) * chunks + chunk, 4)
        return remote(acc.at[lax.rem(chunk, 2), 1], pair_buf.at[slot], ps.at[slot], pr.at[slot], 0)

    def far_sum(chunk):
        return remote(far_src.at[chunk], far_dst.at[chunk], xs.at[chunk], xr.at[chunk], 1)

    def settle(phase, chunk):
        pair_sum(phase, chunk).wait_recv()
        pair_sum(phase, chunk).wait_send()
        slot = lax.rem((1 - phase) * chunks + chunk, 4)
        total = acc[lax.rem(chunk, 2), 0] + pair_buf[slot]
        if phase == 1:
            far_src[chunk] = total
            far_sum(chunk).start()
        else:
            far_sum(chunk).wait_recv()
            cols = pl.ds(pl.multiple_of(chunk * block, block), block)
            out_ref[:, cols] = (hid_ref[:, cols].astype(F32) + total + far_dst[chunk]).astype(BF16)

    for phase in (1, 0):
        def down(chunk, carry, phase=phase):
            down_chunk(phase, chunk)

            @pl.when(chunk > 0)
            def _():
                settle(phase, chunk - 1)

            pair_sum(phase, chunk).start()
            return carry
        lax.fori_loop(0, chunks, down, 0)
        settle(phase, chunks - 1)

    for send in gate_sends:
        send.wait_send()
    pair_send.wait_send()
    for idx in range(u_chunks):
        far_send(idx).wait_send()
        relay_send(idx).wait_send()
    for idx in range(chunks):
        far_sum(idx).wait_send()


def moe(pos_lane, u_own, gates_lane, hidden, w_one, w_three, w_two, onehot, cap):
    seq, model = u_own.shape
    count, _, width = w_one.shape
    u_chunks, chunks, groups, wslots = 4, 8, 4, 4
    block, per = model // chunks, count // groups
    vmem = pl.BlockSpec(memory_space=pltpu.VMEM)
    hbm = pl.BlockSpec(memory_space=pl.ANY)
    dma = pltpu.SemaphoreType.DMA
    return pl.pallas_call(
        functools.partial(moe_kernel, cap=cap, u_chunks=u_chunks, chunks=chunks, groups=groups, wslots=wslots),
        in_specs=[vmem, vmem, vmem, vmem, hbm, hbm, hbm, hbm],
        out_specs=vmem,
        out_shape=jax.ShapeDtypeStruct((seq, model), BF16),
        scratch_shapes=[
            pltpu.VMEM((3, seq, model), BF16), pltpu.VMEM((3, count, seq), F32), pltpu.VMEM((2 * cap, model), BF16),
            pltpu.VMEM((2 * count, 2 * cap, width), BF16), pltpu.VMEM((2, 2 * cap, 128), F32),
            pltpu.VMEM((wslots, 2, model, width // wslots), BF16), pltpu.VMEM((3, per, width, block), BF16),
            pltpu.VMEM((3, 2, seq, per * cap), BF16), pltpu.VMEM((2, 3 * per * cap, block), BF16),
            pltpu.VMEM((2, 2, seq, block), F32), pltpu.VMEM((4, seq, block), F32),
            pltpu.VMEM((chunks, seq, block), F32), pltpu.VMEM((chunks, seq, block), F32),
            dma((1 + 2 * u_chunks,)), dma((1 + 2 * u_chunks,)), dma((3,)), dma((3,)), dma((wslots, 2)), dma((3,)), dma((3,)),
            dma((4,)), dma((4,)), dma((chunks,)), dma((chunks,))],
        compiler_params=pltpu.CompilerParams(collective_id=1, has_side_effects=True, vmem_limit_bytes=67043328),
        name='moe',
    )(pos_lane, u_own, gates_lane, hidden, w_one, w_three, w_two, onehot)


def solution(mesh):
    tok_spec = P(('dp', 'ep'))
    row_spec = P('ep')

    def local_layer(tokens, w_query, w_key, w_value, w_out, w_router, w_one, w_three, w_two, expert_ids):
        seq, model = tokens.shape[1:]
        head_dim = w_query.shape[2]
        choices = expert_ids.shape[2]
        experts = w_router.shape[1]
        own_experts = w_one.shape[0]
        cap = 2 * seq * choices // experts
        group = lax.axis_index('dp')
        me = lax.axis_index('ep')
        x_rows = tokens[0]
        shard = w_out.shape[0]
        half = shard // 2

        pair = functools.partial(lax.ppermute, axis_name='ep', perm=PAIR)
        across = functools.partial(lax.ppermute, axis_name='ep', perm=ACROSS)
        swap = functools.partial(lax.ppermute, axis_name='dp', perm=SWAP)

        def gather(weight):
            mine = lax.dynamic_slice_in_dim(weight, group * half, half, 0).reshape(half, -1)
            full = weight.reshape(shard, -1)
            far = across(mine)
            far_other = swap(far)
            return [full, pair(full), far, far_other, pair(far), pair(far_other)]

        offs = jnp.stack([me * shard, (me ^ 1) * shard,
                          (me ^ 2) * shard + group * half, (me ^ 2) * shard + (1 - group) * half,
                          (me ^ 3) * shard + group * half, (me ^ 3) * shard + (1 - group) * half]).astype(jnp.int32)
        q_parts, k_parts, v_parts, o_parts = [gather(w) for w in (w_query, w_key, w_value, w_out)]

        ids = expert_ids[0]
        ids_pair = pair(ids)
        ids_far = across(ids)
        ids_all = jnp.stack([ids, ids_pair, ids_far, pair(ids_far)])
        mine = me * own_experts + jnp.arange(own_experts, dtype=jnp.int32)
        member = jnp.any(ids_all[:, :, :, None] == mine, axis=2)
        count = member.astype(jnp.int32)
        pos = jnp.where(member, jnp.cumsum(count, axis=1) - count, -1)
        pos_lane = pos.transpose(2, 0, 1)

        normed = rms_norm(x_rows).astype(BF16)
        query = project(offs, normed, q_parts)
        keys = project(offs, normed, k_parts)
        values = project(offs, normed, v_parts)
        context = attend(query, keys, values, head_dim)
        hidden, u_own = out_project(offs, context, x_rows, o_parts)

        logits = jnp.dot(rms_norm(hidden), w_router, precision=lax.Precision.HIGHEST, preferred_element_type=F32)
        chosen = jnp.any(ids[:, :, None] == jnp.arange(experts, dtype=jnp.int32), axis=1)
        gates = jax.nn.softmax(jnp.where(chosen, logits, -jnp.inf), axis=-1)
        return moe(pos_lane, u_own, gates.T, hidden, w_one, w_three, w_two, spread(pos, cap), cap)[None]

    return jax.shard_map(local_layer, mesh=mesh, in_specs=(tok_spec, row_spec, row_spec, row_spec, row_spec, P(), row_spec, row_spec, row_spec, tok_spec), out_specs=tok_spec, check_vma=False)
```

```python
import functools
import jax
import jax.numpy as jnp
from jax import lax
from jax.experimental import pallas as pl
from jax.experimental.pallas import tpu as pltpu
from jax.sharding import PartitionSpec as P

EPS = 1e-6
F32 = jnp.float32
BF16 = jnp.bfloat16


def rms_norm(vals):
    wide = vals.astype(F32)
    return wide * lax.rsqrt(jnp.mean(wide * wide, axis=-1, keepdims=True) + EPS)


def head_attention(q_ref, k_ref, v_ref, out_ref, lanes, rows, scale):
    seq = q_ref.shape[0]
    steps = [slice(start, start + rows) for start in range(0, seq, rows)]
    keep = lax.broadcasted_iota(jnp.int32, (rows, rows), 0) >= lax.broadcasted_iota(jnp.int32, (rows, rows), 1)
    nt_dims = (((1,), (1,)), ((), ()))
    scored = []
    for step in steps:
        tile = q_ref[step, lanes]
        diag = lax.dot_general(tile, k_ref[step, lanes], nt_dims, preferred_element_type=F32)
        parts = [jnp.where(keep, diag, -jnp.inf)]
        if step.start:
            parts.append(lax.dot_general(tile, k_ref[:step.start, lanes], nt_dims, preferred_element_type=F32))
        scored.append(parts)
    weighted = []
    for parts in scored:
        top = functools.reduce(jnp.maximum, [jnp.max(part, axis=-1, keepdims=True) for part in parts])
        expo = [jnp.exp((part - top) * scale) for part in parts]
        total = sum(jnp.sum(part, axis=-1, keepdims=True) for part in expo)
        inverse = 1.0 / total
        weighted.append([(part * inverse).astype(BF16) for part in expo])
    for step, parts in zip(steps, weighted):
        mixed = jnp.dot(parts[0], v_ref[step, lanes], preferred_element_type=F32)
        if step.start:
            mixed += jnp.dot(parts[1], v_ref[:step.start, lanes], preferred_element_type=F32)
        out_ref[step, lanes] = mixed.astype(BF16)


def front_kernel(ids_ref, x_ref, wq_ref, wk_ref, wv_ref, wo_ref, hid_ref, u_ref, pos_ref, oh_ref,
                 full, normed, qkv, ctx, ids_all, oh_buf,
                 own_s, po_s, po_r, xs, xr, ys, yr, rs, rr, ids_s, ids_r, oh_s, *, subs, cap, count, head_dim):
    group, me = lax.axis_index('dp'), lax.axis_index('ep')
    weights = (wq_ref, wk_ref, wv_ref, wo_ref)
    shard, model = wo_ref.shape
    seq = x_ref.shape[0]
    half, rows, cols = shard // 2, shard // 2 // subs, model // 2
    order = [(0, 0), (1, 0), (2, 0), (0, 1), (1, 1), (2, 1), (3, 0), (3, 1)]
    heads = model // head_dim

    def remote(src, dst, send, recv, where):
        return pltpu.make_async_remote_copy(src_ref=src, dst_ref=dst, send_sem=send, recv_sem=recv,
                                            device_id=where, device_id_type=pl.DeviceIdType.MESH)

    def block(stage, source, which, sub):
        matrix, side = order[stage]
        start = pl.multiple_of(source * shard + which * half + sub * rows, rows)
        return full.at[matrix, pl.ds(start, rows), pl.ds(side * cols, cols)]

    def own_rows(matrix):
        return full.at[matrix, pl.ds(pl.multiple_of(me * shard, shard), shard)]

    def own_local(matrix):
        return pltpu.make_async_copy(weights[matrix], own_rows(matrix), own_s.at[matrix])

    def own_pair(matrix):
        return remote(weights[matrix], own_rows(matrix), po_s.at[matrix], po_r.at[matrix], {'ep': me ^ 1})

    def x_copy(stage, sub):
        matrix, side = order[stage]
        src = weights[matrix].at[pl.ds(pl.multiple_of(group * half + sub * rows, rows), rows), pl.ds(side * cols, cols)]
        sem = stage * subs + sub
        return remote(src, block(stage, me, group, sub), xs.at[sem], xr.at[sem], {'ep': me ^ 2})

    def y_copy(stage, sub):
        ref = block(stage, me ^ 2, group, sub)
        sem = stage * subs + sub
        return remote(ref, ref, ys.at[sem], yr.at[sem], {'dp': 1 - group})

    def relay(stage, sub, other):
        ref = block(stage, me ^ 2, 1 - group if other else group, sub)
        sem = (stage * subs + sub) * 2 + other
        return remote(ref, ref, rs.at[sem], rr.at[sem], {'ep': me ^ 1})

    def ids_copy(relation):
        return remote(ids_ref, ids_all.at[relation - 1], ids_s.at[relation - 1], ids_r.at[relation - 1], {'ep': me ^ relation})

    def oh_copy(source):
        return pltpu.make_async_copy(oh_buf.at[source % 2], oh_ref.at[source], oh_s.at[source % 2])

    barrier = pltpu.get_barrier_semaphore()
    for peer in ({'ep': me ^ 1}, {'ep': me ^ 2}, {'ep': me ^ 3}, {'dp': 1 - group}):
        pl.semaphore_signal(barrier, inc=1, device_id=peer, device_id_type=pl.DeviceIdType.MESH)
    pl.semaphore_wait(barrier, 4)

    for relation in (1, 2, 3):
        ids_copy(relation).start()
    messages = [(stage, sub) for stage in range(len(order)) for sub in range(subs)]
    for message in messages:
        x_copy(*message).start()
    for matrix in range(4):
        own_pair(matrix).start()
        own_local(matrix).start()

    normed[...] = rms_norm(x_ref[...]).astype(BF16)

    def place_tokens():
        for relation in (1, 2, 3):
            ids_copy(relation).wait_recv()
        mine = lax.broadcasted_iota(jnp.int32, (count, seq), 0) + me * count
        earlier = (lax.broadcasted_iota(jnp.int32, (seq, seq), 0) < lax.broadcasted_iota(jnp.int32, (seq, seq), 1))
        earlier = earlier.astype(F32).astype(BF16)
        places = []
        for source in range(4):
            ids = ids_ref[...] if source == 0 else ids_all[source - 1]
            member = mine == ids[0:1, :]
            for choice in range(1, ids.shape[0]):
                member = jnp.logical_or(member, mine == ids[choice:choice + 1, :])
            before = jnp.dot(member.astype(F32).astype(BF16), earlier, preferred_element_type=F32)
            places.append(jnp.where(member, before, -1.0))
            pos_ref[source] = places[source].astype(jnp.int32)
        filler = jnp.zeros((128 - 4 * count, seq), F32)
        by_token = jnp.concatenate(places + [filler], axis=0).T
        slots = lax.broadcasted_iota(jnp.int32, (seq, cap), 1).astype(F32)
        for source in range(4):
            if source >= 2:
                oh_copy(source - 2).wait()
            for expert in range(count):
                lane = source * count + expert
                hit = by_token[:, lane:lane + 1] == slots
                oh_buf[source % 2, :, expert * cap:(expert + 1) * cap] = hit.astype(F32).astype(BF16)
            oh_copy(source).start()

    def ready(stage):
        matrix, side = order[stage]
        if side == 0:
            own_local(matrix).wait()
            own_pair(matrix).wait_recv()
        for sub in range(subs):
            relay(stage, sub, 0).wait_recv()
            relay(stage, sub, 1).wait_recv()

    def project(stage):
        matrix, side = order[stage]

        def body(idx, carry):
            lanes = pl.ds(pl.multiple_of(side * cols + idx * 256, 256), 256)
            qkv[matrix, :, lanes] = jnp.dot(normed[...], full[matrix, :, lanes], preferred_element_type=F32).astype(BF16)
            return carry
        lax.fori_loop(0, cols // 256, body, 0)

    def attend(first, last):
        def body(head, carry):
            lanes = pl.ds(pl.multiple_of(head * head_dim, head_dim), head_dim)
            head_attention(qkv.at[0], qkv.at[1], qkv.at[2], ctx, lanes, 128, head_dim ** -0.5)
            return carry
        lax.fori_loop(first, last, body, 0)

    def combine(stage):
        side = order[stage][1]

        def body(idx, carry):
            lanes = pl.ds(pl.multiple_of(side * cols + idx * 256, 256), 256)
            mixed = jnp.dot(ctx[...], full[3, :, lanes], preferred_element_type=F32)
            hid_ref[:, lanes] = (x_ref[:, lanes].astype(F32) + mixed).astype(BF16)
            return carry
        lax.fori_loop(0, cols // 256, body, 0)

    def work(stage, sub):
        if (stage, sub) == (0, 0):
            place_tokens()
        if sub == 0 and stage > 0:
            ready(stage - 1)
            if stage - 1 < 6:
                project(stage - 1)
        quarter = heads // 8
        if sub == subs - 1 and 3 <= stage <= 5:
            first = (0, 3, 6)[stage - 3] * quarter // 2
            attend(first, min(first + 3 * quarter // 2, heads // 2))
        if stage == 6:
            attend(heads // 2 + sub * quarter, heads // 2 + (sub + 1) * quarter)
        if stage == 7 and sub == 0:
            attend(heads // 2 + subs * quarter, heads)
            combine(6)

    previous = None
    for message in messages:
        x_copy(*message).wait_recv()
        y_copy(*message).start()
        relay(*message, 0).start()
        if previous is not None:
            y_copy(*previous).wait_recv()
            relay(*previous, 1).start()
        work(*message)
        previous = message
    y_copy(*previous).wait_recv()
    relay(*previous, 1).start()
    ready(7)
    combine(7)
    u_ref[...] = rms_norm(hid_ref[...]).astype(BF16)

    oh_copy(2).wait()
    oh_copy(3).wait()
    for relation in (1, 2, 3):
        ids_copy(relation).wait_send()
    for matrix in range(4):
        own_pair(matrix).wait_send()
    for message in messages:
        x_copy(*message).wait_send()
        y_copy(*message).wait_send()
        relay(*message, 0).wait_send()
        relay(*message, 1).wait_send()


def front(ids_lane, tokens, w_query, w_key, w_value, w_out, cap, count, head_dim):
    seq, model = tokens.shape
    subs = 2
    vmem = pl.BlockSpec(memory_space=pltpu.VMEM)
    hbm = pl.BlockSpec(memory_space=pl.ANY)
    dma = pltpu.SemaphoreType.DMA
    sends = 8 * subs
    return pl.pallas_call(
        functools.partial(front_kernel, subs=subs, cap=cap, count=count, head_dim=head_dim),
        in_specs=[vmem, vmem, hbm, hbm, hbm, hbm],
        out_specs=[vmem, vmem, vmem, hbm],
        out_shape=[jax.ShapeDtypeStruct((seq, model), BF16), jax.ShapeDtypeStruct((seq, model), BF16),
                   jax.ShapeDtypeStruct((4, count, seq), jnp.int32), jax.ShapeDtypeStruct((4, seq, count * cap), BF16)],
        scratch_shapes=[
            pltpu.VMEM((4, model, model), BF16), pltpu.VMEM((seq, model), BF16), pltpu.VMEM((3, seq, model), BF16),
            pltpu.VMEM((seq, model), BF16), pltpu.VMEM((3,) + ids_lane.shape, jnp.int32), pltpu.VMEM((2, seq, count * cap), BF16),
            dma((4,)), dma((4,)), dma((4,)), dma((sends,)), dma((sends,)), dma((sends,)), dma((sends,)),
            dma((2 * sends,)), dma((2 * sends,)), dma((3,)), dma((3,)), dma((2,))],
        compiler_params=pltpu.CompilerParams(collective_id=2, has_side_effects=True, vmem_limit_bytes=67043328),
        name='front',
    )(ids_lane, tokens, w_query, w_key, w_value, w_out)


def moe_kernel(pos_ref, u_ref, gate_ref, hid_ref, w1_ref, w3_ref, w2_ref, oh_ref, out_ref,
               ug, gg, rows, act, gcol, w13, w2t, oht, pst, acc, pair_buf, far_src, far_dst,
               us, ur, gs, gr, ws, w2s, ohs, ps, pr, xs, xr,
               *, cap, u_chunks, chunks, groups, wslots):
    me = lax.axis_index('ep')
    relations = (me ^ 1, me ^ 2, me ^ 3)
    seq, model = u_ref.shape
    count, _, width = w1_ref.shape
    col = width // wslots
    block = model // chunks
    per = count // groups
    piece = seq // u_chunks

    def remote(src, dst, send, recv, relation):
        return pltpu.make_async_remote_copy(src_ref=src, dst_ref=dst, send_sem=send, recv_sem=recv,
                                            device_id={'ep': relations[relation]}, device_id_type=pl.DeviceIdType.MESH)

    def w13_copy(expert, slot, which):
        ref = (w1_ref, w3_ref)[which]
        return pltpu.make_async_copy(ref.at[expert, :, pl.ds(slot * col, col)], w13.at[slot, which], ws.at[slot, which])

    def w2_copy(chunk, part, slot):
        return pltpu.make_async_copy(w2_ref.at[pl.ds(part * per, per), :, pl.ds(pl.multiple_of(chunk * block, block), block)],
                                     w2t.at[slot], w2s.at[slot])

    def oh_copy(phase, part, slot):
        return pltpu.make_async_copy(oh_ref.at[pl.ds(2 * phase, 2), :, pl.ds(part * per * cap, per * cap)],
                                     oht.at[slot], ohs.at[slot])

    for slot in range(wslots):
        w13_copy(0, slot, 0).start()
        w13_copy(0, slot, 1).start()

    barrier = pltpu.get_barrier_semaphore()
    for peer in relations:
        pl.semaphore_signal(barrier, inc=1, device_id={'ep': peer}, device_id_type=pl.DeviceIdType.MESH)
    pl.semaphore_wait(barrier, 3)

    gate_sends = [remote(gate_ref.at[pl.ds(pl.multiple_of(relations[r] * count, count), count)], gg.at[r], gs.at[r], gr.at[r], r)
                  for r in range(3)]
    pair_send = remote(u_ref, ug.at[0], us.at[0], ur.at[0], 0)

    def far_send(idx):
        part = pl.ds(idx * piece, piece)
        return remote(u_ref.at[part], ug.at[1, part], us.at[1 + idx], ur.at[1 + idx], 1)

    def relay_send(idx):
        part = pl.ds(idx * piece, piece)
        return remote(ug.at[1, part], ug.at[2, part], us.at[1 + u_chunks + idx], ur.at[1 + u_chunks + idx], 0)

    for send in gate_sends:
        send.start()
    for idx in range(u_chunks):
        far_send(idx).start()
    pair_send.start()

    slots = lax.broadcasted_iota(jnp.int32, (cap, seq), 0)
    lanes = lax.broadcasted_iota(jnp.int32, (2 * cap, 128), 1)

    def up_step(phase, expert):
        if phase == 0:
            sources = ((u_ref[...], gate_ref[pl.ds(me * count + expert, 1), :]), (ug[0], gg[0, pl.ds(expert, 1), :]))
        else:
            sources = ((ug[1], gg[1, pl.ds(expert, 1), :]), (ug[2], gg[2, pl.ds(expert, 1), :]))
        for src, (u_val, gate_row) in enumerate(sources):
            hit = pos_ref[2 * phase + src, pl.ds(expert, 1), :] == slots
            rows[src * cap:(src + 1) * cap, :] = jnp.dot(hit.astype(F32).astype(BF16), u_val,
                                                         preferred_element_type=F32).astype(BF16)
            column = jnp.sum(jnp.where(hit, gate_row, 0.0), axis=-1, keepdims=True)
            part = slice(src * cap, (src + 1) * cap)
            gcol[phase, part, :] = jnp.where(lanes[part] == expert, column, gcol[phase, part, :])
        for slot in range(wslots):
            w13_copy(0, slot, 0).wait()
            w13_copy(0, slot, 1).wait()
            first = jnp.dot(rows[...], w13[slot, 0], preferred_element_type=F32)
            third = jnp.dot(rows[...], w13[slot, 1], preferred_element_type=F32)
            act[phase * count + expert, :, slot * col:(slot + 1) * col] = (jax.nn.silu(first) * third).astype(BF16)

            def refill(slot=slot):
                following = lax.rem(expert + 1, count)
                w13_copy(following, slot, 0).start()
                w13_copy(following, slot, 1).start()

            if phase == 0:
                refill()
            else:
                pl.when(expert < count - 1)(refill)

    gcol[...] = jnp.zeros_like(gcol)
    gate_sends[0].wait_recv()
    pair_send.wait_recv()
    step = count // u_chunks
    for idx in range(u_chunks):
        def near(expert, carry):
            up_step(0, expert)
            return carry
        lax.fori_loop(idx * step, (idx + 1) * step, near, 0)
        far_send(idx).wait_recv()
        relay_send(idx).start()
    for idx in range(3):
        w2_copy(0, idx, idx).start()
        oh_copy(1, idx, idx).start()
    gate_sends[1].wait_recv()
    gate_sends[2].wait_recv()
    for idx in range(u_chunks):
        relay_send(idx).wait_recv()

    def away(expert, carry):
        up_step(1, expert)
        return carry
    lax.fori_loop(0, count, away, 0)

    def down_chunk(phase, chunk):
        order = (1 - phase) * chunks + chunk
        for part in range(groups):
            slot = lax.rem(order * groups + part, 3)
            w2_copy(0, 0, slot).wait()
            oh_copy(0, 0, slot).wait()
            for idx in range(per):
                expert = part * per + idx
                done = jnp.dot(act[phase * count + expert], w2t[slot, idx], preferred_element_type=F32).astype(BF16)
                rest = done.astype(F32) * gcol[phase, :, expert:expert + 1]
                for term in range(3):
                    head = rest.astype(BF16)
                    at = (term * per + idx) * cap
                    pst[0, at:at + cap, :] = head[:cap]
                    pst[1, at:at + cap, :] = head[cap:]
                    rest = rest - head.astype(F32)
            depth = per * cap
            for src in range(2):
                mixed = jnp.dot(oht[slot, src], pst[src, 0:depth, :], preferred_element_type=F32)
                for term in range(1, 3):
                    mixed += jnp.dot(oht[slot, src], pst[src, term * depth:(term + 1) * depth, :], preferred_element_type=F32)
                if part == 0:
                    acc[lax.rem(chunk, 2), src] = mixed
                else:
                    acc[lax.rem(chunk, 2), src] += mixed

            def refill(part=part, slot=slot):
                ahead = order * groups + part + 3
                ahead_chunk = lax.rem(ahead // groups, chunks)
                ahead_part = lax.rem(ahead, groups)
                ahead_phase = 1 - ahead // (groups * chunks)
                w2_copy(ahead_chunk, ahead_part, slot).start()
                oh_copy(ahead_phase, ahead_part, slot).start()

            if phase == 1:
                refill()
            else:
                pl.when(order * groups + part + 3 < 2 * groups * chunks)(refill)

    def pair_sum(phase, chunk):
        slot = lax.rem((1 - phase) * chunks + chunk, 4)
        return remote(acc.at[lax.rem(chunk, 2), 1], pair_buf.at[slot], ps.at[slot], pr.at[slot], 0)

    def far_sum(chunk):
        return remote(far_src.at[chunk], far_dst.at[chunk], xs.at[chunk], xr.at[chunk], 1)

    def settle(phase, chunk):
        pair_sum(phase, chunk).wait_recv()
        pair_sum(phase, chunk).wait_send()
        slot = lax.rem((1 - phase) * chunks + chunk, 4)
        total = acc[lax.rem(chunk, 2), 0] + pair_buf[slot]
        if phase == 1:
            far_src[chunk] = total
            far_sum(chunk).start()
        else:
            far_sum(chunk).wait_recv()
            cols = pl.ds(pl.multiple_of(chunk * block, block), block)
            out_ref[:, cols] = (hid_ref[:, cols].astype(F32) + total + far_dst[chunk]).astype(BF16)

    for phase in (1, 0):
        def down(chunk, carry, phase=phase):
            down_chunk(phase, chunk)

            @pl.when(chunk > 0)
            def _():
                settle(phase, chunk - 1)

            pair_sum(phase, chunk).start()
            return carry
        lax.fori_loop(0, chunks, down, 0)
        settle(phase, chunks - 1)

    for send in gate_sends:
        send.wait_send()
    pair_send.wait_send()
    for idx in range(u_chunks):
        far_send(idx).wait_send()
        relay_send(idx).wait_send()
    for idx in range(chunks):
        far_sum(idx).wait_send()


def moe(pos_lane, u_own, gates_lane, hidden, w_one, w_three, w_two, onehot, cap):
    seq, model = u_own.shape
    count, _, width = w_one.shape
    u_chunks, chunks, groups, wslots = 4, 8, 4, 4
    block, per = model // chunks, count // groups
    vmem = pl.BlockSpec(memory_space=pltpu.VMEM)
    hbm = pl.BlockSpec(memory_space=pl.ANY)
    dma = pltpu.SemaphoreType.DMA
    return pl.pallas_call(
        functools.partial(moe_kernel, cap=cap, u_chunks=u_chunks, chunks=chunks, groups=groups, wslots=wslots),
        in_specs=[vmem, vmem, vmem, vmem, hbm, hbm, hbm, hbm],
        out_specs=vmem,
        out_shape=jax.ShapeDtypeStruct((seq, model), BF16),
        scratch_shapes=[
            pltpu.VMEM((3, seq, model), BF16), pltpu.VMEM((3, count, seq), F32), pltpu.VMEM((2 * cap, model), BF16),
            pltpu.VMEM((2 * count, 2 * cap, width), BF16), pltpu.VMEM((2, 2 * cap, 128), F32),
            pltpu.VMEM((wslots, 2, model, width // wslots), BF16), pltpu.VMEM((3, per, width, block), BF16),
            pltpu.VMEM((3, 2, seq, per * cap), BF16), pltpu.VMEM((2, 3 * per * cap, block), BF16),
            pltpu.VMEM((2, 2, seq, block), F32), pltpu.VMEM((4, seq, block), F32),
            pltpu.VMEM((chunks, seq, block), F32), pltpu.VMEM((chunks, seq, block), F32),
            dma((1 + 2 * u_chunks,)), dma((1 + 2 * u_chunks,)), dma((3,)), dma((3,)), dma((wslots, 2)), dma((3,)), dma((3,)),
            dma((4,)), dma((4,)), dma((chunks,)), dma((chunks,))],
        compiler_params=pltpu.CompilerParams(collective_id=1, has_side_effects=True, vmem_limit_bytes=67043328),
        name='moe',
    )(pos_lane, u_own, gates_lane, hidden, w_one, w_three, w_two, onehot)


def solution(mesh):
    tok_spec = P(('dp', 'ep'))
    row_spec = P('ep')

    def local_layer(tokens, w_query, w_key, w_value, w_out, w_router, w_one, w_three, w_two, expert_ids):
        seq, model = tokens.shape[1:]
        head_dim = w_query.shape[2]
        choices = expert_ids.shape[2]
        experts = w_router.shape[1]
        own_experts = w_one.shape[0]
        cap = 2 * seq * choices // experts
        ids = expert_ids[0]
        flat = [w.reshape(w.shape[0], -1) for w in (w_query, w_key, w_value)]
        hidden, u_own, pos, onehot = front(ids.T, tokens[0], *flat, w_out, cap, own_experts, head_dim)
        logits = jnp.dot(rms_norm(hidden), w_router, precision=lax.Precision.HIGHEST, preferred_element_type=F32)
        chosen = jnp.any(ids[:, :, None] == jnp.arange(experts, dtype=jnp.int32), axis=1)
        gates = jax.nn.softmax(jnp.where(chosen, logits, -jnp.inf), axis=-1)
        return moe(pos, u_own, gates.T, hidden, w_one, w_three, w_two, onehot, cap)[None]

    return jax.shard_map(local_layer, mesh=mesh, in_specs=(tok_spec, row_spec, row_spec, row_spec, row_spec, P(), row_spec, row_spec, row_spec, tok_spec), out_specs=tok_spec, check_vma=False)
```

```python
import functools
import jax
import jax.numpy as jnp
from jax import lax
from jax.experimental import pallas as pl
from jax.experimental.pallas import tpu as pltpu
from jax.sharding import PartitionSpec as P

EPS = 1e-6
F32 = jnp.float32
BF16 = jnp.bfloat16


def rms_norm(vals):
    wide = vals.astype(F32)
    return wide * lax.rsqrt(jnp.mean(wide * wide, axis=-1, keepdims=True) + EPS)


def head_attention(q_ref, k_ref, v_ref, out_ref, lanes, rows, scale):
    seq = q_ref.shape[0]
    steps = [slice(start, start + rows) for start in range(0, seq, rows)]
    keep = lax.broadcasted_iota(jnp.int32, (rows, rows), 0) >= lax.broadcasted_iota(jnp.int32, (rows, rows), 1)
    nt_dims = (((1,), (1,)), ((), ()))
    scored = []
    for step in steps:
        tile = q_ref[step, lanes]
        diag = lax.dot_general(tile, k_ref[step, lanes], nt_dims, preferred_element_type=F32)
        parts = [jnp.where(keep, diag, -jnp.inf)]
        if step.start:
            parts.append(lax.dot_general(tile, k_ref[:step.start, lanes], nt_dims, preferred_element_type=F32))
        scored.append(parts)
    weighted = []
    for parts in scored:
        top = functools.reduce(jnp.maximum, [jnp.max(part, axis=-1, keepdims=True) for part in parts])
        expo = [jnp.exp((part - top) * scale) for part in parts]
        total = sum(jnp.sum(part, axis=-1, keepdims=True) for part in expo)
        inverse = 1.0 / total
        weighted.append([(part * inverse).astype(BF16) for part in expo])
    for step, parts in zip(steps, weighted):
        mixed = jnp.dot(parts[0], v_ref[step, lanes], preferred_element_type=F32)
        if step.start:
            mixed += jnp.dot(parts[1], v_ref[:step.start, lanes], preferred_element_type=F32)
        out_ref[step, lanes] = mixed.astype(BF16)


def front_kernel(ids_ref, x_ref, wq_ref, wk_ref, wv_ref, wo_ref, hid_ref, u_ref, pos_ref, oh_ref,
                 full, normed, qkv, ctx, ids_all, oh_buf,
                 own_s, po_s, po_r, xs, xr, ys, yr, rs, rr, ids_s, ids_r, oh_s, *, subs, cap, count, head_dim):
    group, me = lax.axis_index('dp'), lax.axis_index('ep')
    weights = (wq_ref, wk_ref, wv_ref, wo_ref)
    shard, model = wo_ref.shape
    seq = x_ref.shape[0]
    half, rows, cols = shard // 2, shard // 2 // subs, model // 2
    order = [(0, 0), (1, 0), (2, 0), (0, 1), (1, 1), (2, 1), (3, 0), (3, 1)]
    heads = model // head_dim

    def remote(src, dst, send, recv, where):
        return pltpu.make_async_remote_copy(src_ref=src, dst_ref=dst, send_sem=send, recv_sem=recv,
                                            device_id=where, device_id_type=pl.DeviceIdType.MESH)

    def block(stage, source, which, sub):
        matrix, side = order[stage]
        start = pl.multiple_of(source * shard + which * half + sub * rows, rows)
        return full.at[matrix, pl.ds(start, rows), pl.ds(side * cols, cols)]

    def own_rows(matrix):
        return full.at[matrix, pl.ds(pl.multiple_of(me * shard, shard), shard)]

    def own_local(matrix):
        return pltpu.make_async_copy(weights[matrix], own_rows(matrix), own_s.at[matrix])

    def own_pair(matrix):
        return remote(weights[matrix], own_rows(matrix), po_s.at[matrix], po_r.at[matrix], {'ep': me ^ 1})

    def x_copy(stage, sub):
        matrix, side = order[stage]
        src = weights[matrix].at[pl.ds(pl.multiple_of(group * half + sub * rows, rows), rows), pl.ds(side * cols, cols)]
        sem = stage * subs + sub
        return remote(src, block(stage, me, group, sub), xs.at[sem], xr.at[sem], {'ep': me ^ 2})

    def y_copy(stage, sub):
        ref = block(stage, me ^ 2, group, sub)
        sem = stage * subs + sub
        return remote(ref, ref, ys.at[sem], yr.at[sem], {'dp': 1 - group})

    def relay(stage, sub, other):
        ref = block(stage, me ^ 2, 1 - group if other else group, sub)
        sem = (stage * subs + sub) * 2 + other
        return remote(ref, ref, rs.at[sem], rr.at[sem], {'ep': me ^ 1})

    def ids_copy(relation):
        return remote(ids_ref, ids_all.at[relation - 1], ids_s.at[relation - 1], ids_r.at[relation - 1], {'ep': me ^ relation})

    def oh_copy(source):
        return pltpu.make_async_copy(oh_buf.at[source % 2], oh_ref.at[source], oh_s.at[source % 2])

    barrier = pltpu.get_barrier_semaphore()
    for peer in ({'ep': me ^ 1}, {'ep': me ^ 2}, {'ep': me ^ 3}, {'dp': 1 - group}):
        pl.semaphore_signal(barrier, inc=1, device_id=peer, device_id_type=pl.DeviceIdType.MESH)
    pl.semaphore_wait(barrier, 4)

    for relation in (1, 2, 3):
        ids_copy(relation).start()
    messages = [(stage, sub) for stage in range(len(order)) for sub in range(subs)]
    for message in messages:
        x_copy(*message).start()
    for matrix in range(4):
        own_pair(matrix).start()
        own_local(matrix).start()

    normed[...] = rms_norm(x_ref[...]).astype(BF16)

    def place_tokens():
        for relation in (1, 2, 3):
            ids_copy(relation).wait_recv()
        mine = lax.broadcasted_iota(jnp.int32, (count, seq), 0) + me * count
        earlier = (lax.broadcasted_iota(jnp.int32, (seq, seq), 0) < lax.broadcasted_iota(jnp.int32, (seq, seq), 1))
        earlier = earlier.astype(F32).astype(BF16)
        places = []
        for source in range(4):
            ids = ids_ref[...] if source == 0 else ids_all[source - 1]
            member = mine == ids[0:1, :]
            for choice in range(1, ids.shape[0]):
                member = jnp.logical_or(member, mine == ids[choice:choice + 1, :])
            before = jnp.dot(member.astype(F32).astype(BF16), earlier, preferred_element_type=F32)
            places.append(jnp.where(member, before, -1.0))
            pos_ref[source] = places[source].astype(jnp.int32)
        filler = jnp.zeros((128 - 4 * count, seq), F32)
        by_token = jnp.concatenate(places + [filler], axis=0).T
        slots = lax.broadcasted_iota(jnp.int32, (seq, cap), 1).astype(F32)
        for source in range(4):
            if source >= 2:
                oh_copy(source - 2).wait()
            for expert in range(count):
                lane = source * count + expert
                hit = by_token[:, lane:lane + 1] == slots
                oh_buf[source % 2, :, expert * cap:(expert + 1) * cap] = hit.astype(F32).astype(BF16)
            oh_copy(source).start()

    def ready(stage):
        matrix, side = order[stage]
        if side == 0:
            own_local(matrix).wait()
            own_pair(matrix).wait_recv()
        for sub in range(subs):
            relay(stage, sub, 0).wait_recv()
            relay(stage, sub, 1).wait_recv()

    def project(stage):
        matrix, side = order[stage]

        def body(idx, carry):
            lanes = pl.ds(pl.multiple_of(side * cols + idx * 256, 256), 256)
            qkv[matrix, :, lanes] = jnp.dot(normed[...], full[matrix, :, lanes], preferred_element_type=F32).astype(BF16)
            return carry
        lax.fori_loop(0, cols // 256, body, 0)

    def attend(first, last):
        def body(head, carry):
            lanes = pl.ds(pl.multiple_of(head * head_dim, head_dim), head_dim)
            head_attention(qkv.at[0], qkv.at[1], qkv.at[2], ctx, lanes, 128, head_dim ** -0.5)
            return carry
        lax.fori_loop(first, last, body, 0)

    def combine(stage):
        side = order[stage][1]

        def body(idx, carry):
            lanes = pl.ds(pl.multiple_of(side * cols + idx * 256, 256), 256)
            mixed = jnp.dot(ctx[...], full[3, :, lanes], preferred_element_type=F32)
            hid_ref[:, lanes] = (x_ref[:, lanes].astype(F32) + mixed).astype(BF16)
            return carry
        lax.fori_loop(0, cols // 256, body, 0)

    def work(stage, sub):
        if (stage, sub) == (0, 0):
            place_tokens()
        if sub == 0 and stage > 0:
            ready(stage - 1)
            if stage - 1 < 6:
                project(stage - 1)
        quarter = heads // 8
        if sub == subs - 1 and 3 <= stage <= 5:
            first = (0, 3, 6)[stage - 3] * quarter // 2
            attend(first, min(first + 3 * quarter // 2, heads // 2))
        if stage == 6:
            attend(heads // 2 + sub * quarter, heads // 2 + (sub + 1) * quarter)
        if stage == 7 and sub == 0:
            attend(heads // 2 + subs * quarter, heads)
            combine(6)

    previous = None
    for message in messages:
        x_copy(*message).wait_recv()
        y_copy(*message).start()
        relay(*message, 0).start()
        if previous is not None:
            y_copy(*previous).wait_recv()
            relay(*previous, 1).start()
        work(*message)
        previous = message
    y_copy(*previous).wait_recv()
    relay(*previous, 1).start()
    ready(7)
    combine(7)
    u_ref[...] = rms_norm(hid_ref[...]).astype(BF16)

    oh_copy(2).wait()
    oh_copy(3).wait()
    for relation in (1, 2, 3):
        ids_copy(relation).wait_send()
    for matrix in range(4):
        own_pair(matrix).wait_send()
    for message in messages:
        x_copy(*message).wait_send()
        y_copy(*message).wait_send()
        relay(*message, 0).wait_send()
        relay(*message, 1).wait_send()


def front(ids_lane, tokens, w_query, w_key, w_value, w_out, cap, count, head_dim):
    seq, model = tokens.shape
    subs = 4
    vmem = pl.BlockSpec(memory_space=pltpu.VMEM)
    hbm = pl.BlockSpec(memory_space=pl.ANY)
    dma = pltpu.SemaphoreType.DMA
    sends = 8 * subs
    return pl.pallas_call(
        functools.partial(front_kernel, subs=subs, cap=cap, count=count, head_dim=head_dim),
        in_specs=[vmem, vmem, hbm, hbm, hbm, hbm],
        out_specs=[vmem, vmem, vmem, hbm],
        out_shape=[jax.ShapeDtypeStruct((seq, model), BF16), jax.ShapeDtypeStruct((seq, model), BF16),
                   jax.ShapeDtypeStruct((4, count, seq), jnp.int32), jax.ShapeDtypeStruct((4, seq, count * cap), BF16)],
        scratch_shapes=[
            pltpu.VMEM((4, model, model), BF16), pltpu.VMEM((seq, model), BF16), pltpu.VMEM((3, seq, model), BF16),
            pltpu.VMEM((seq, model), BF16), pltpu.VMEM((3,) + ids_lane.shape, jnp.int32), pltpu.VMEM((2, seq, count * cap), BF16),
            dma((4,)), dma((4,)), dma((4,)), dma((sends,)), dma((sends,)), dma((sends,)), dma((sends,)),
            dma((2 * sends,)), dma((2 * sends,)), dma((3,)), dma((3,)), dma((2,))],
        compiler_params=pltpu.CompilerParams(collective_id=2, has_side_effects=True, vmem_limit_bytes=67043328),
        name='front',
    )(ids_lane, tokens, w_query, w_key, w_value, w_out)


def moe_kernel(pos_ref, u_ref, gate_ref, hid_ref, w1_ref, w3_ref, w2_ref, oh_ref, out_ref,
               ug, gg, rows, act, gcol, pool, oht, pst, acc, pair_buf, far_src, far_dst,
               us, ur, gs, gr, ws, ohs, ps, pr, xs, xr,
               *, cap, u_chunks, chunks, groups, wslots):
    me = lax.axis_index('ep')
    relations = (me ^ 1, me ^ 2, me ^ 3)
    seq, model = u_ref.shape
    count, _, width = w1_ref.shape
    col = width // wslots
    block = model // chunks
    per = count // groups
    piece = seq // u_chunks

    def remote(src, dst, send, recv, relation):
        return pltpu.make_async_remote_copy(src_ref=src, dst_ref=dst, send_sem=send, recv_sem=recv,
                                            device_id={'ep': relations[relation]}, device_id_type=pl.DeviceIdType.MESH)

    ring = pool.shape[0]
    up_tiles = 2 * count * wslots

    def w13_copies(tile):
        slot, expert = lax.rem(tile, ring), lax.rem(tile // wslots, count)
        at = pl.multiple_of(lax.rem(tile, wslots) * col, col)
        return [pltpu.make_async_copy(ref.at[expert, :, pl.ds(at, col)], pool.at[slot, :, pl.ds(which * col, col)], ws.at[slot, which])
                for which, ref in enumerate((w1_ref, w3_ref))]

    def w2_copies(step):
        slot = lax.rem(step + up_tiles, ring)
        at = pl.multiple_of(lax.rem(step // groups, chunks) * block, block)
        return [pltpu.make_async_copy(w2_ref.at[lax.rem(step, groups) * per + idx, :, pl.ds(at, block)],
                                      pool.at[slot, pl.ds(idx * width, width), :], ws.at[slot, idx]) for idx in range(per)]

    def w13_start(tile):
        for copy in w13_copies(tile):
            copy.start()

    def w2_start(step):
        for copy in w2_copies(step):
            copy.start()

    def oh_copy(step):
        slot = lax.rem(step, 3)
        phase = 1 - step // (groups * chunks)
        depth = per * cap
        return pltpu.make_async_copy(oh_ref.at[pl.ds(2 * phase, 2), :,
                                               pl.ds(pl.multiple_of(lax.rem(step, groups) * depth, depth), depth)],
                                     oht.at[slot], ohs.at[slot])

    for tile in range(ring):
        w13_start(tile)

    barrier = pltpu.get_barrier_semaphore()
    for peer in relations:
        pl.semaphore_signal(barrier, inc=1, device_id={'ep': peer}, device_id_type=pl.DeviceIdType.MESH)
    pl.semaphore_wait(barrier, 3)

    gate_sends = [remote(gate_ref.at[pl.ds(pl.multiple_of(relations[r] * count, count), count)], gg.at[r], gs.at[r], gr.at[r], r)
                  for r in range(3)]
    pair_send = remote(u_ref, ug.at[0], us.at[0], ur.at[0], 0)

    def far_send(idx):
        part = pl.ds(pl.multiple_of(idx * piece, piece), piece)
        return remote(u_ref.at[part], ug.at[1, part], us.at[1 + idx], ur.at[1 + idx], 1)

    def relay_send(idx):
        part = pl.ds(pl.multiple_of(idx * piece, piece), piece)
        return remote(ug.at[1, part], ug.at[2, part], us.at[1 + u_chunks + idx], ur.at[1 + u_chunks + idx], 0)

    for send in gate_sends:
        send.start()
    for idx in range(u_chunks):
        far_send(idx).start()
    pair_send.start()

    slots = lax.broadcasted_iota(jnp.int32, (cap, seq), 0)
    lanes = lax.broadcasted_iota(jnp.int32, (cap, 128), 1)

    def up_step(phase, index):
        first_expert = 2 * index
        first_tile = (phase * count + first_expert) * wslots
        if phase == 0:
            sources = ((u_ref, gate_ref, me * count), (ug.at[0], gg.at[0], 0))
        else:
            sources = ((ug.at[1], gg.at[1], 0), (ug.at[2], gg.at[2], 0))

        def gather():
            for src, (tokens_ref, gates_ref, offset) in enumerate(sources):
                part = slice(src * cap, (src + 1) * cap)
                picks = []
                for idx in range(2):
                    hit = pos_ref[2 * phase + src, pl.ds(first_expert + idx, 1), :] == slots
                    picks.append(hit.astype(F32).astype(BF16))
                    gate_row = gates_ref[pl.ds(offset + first_expert + idx, 1), :]
                    column = jnp.sum(jnp.where(hit, gate_row, 0.0), axis=-1, keepdims=True)
                    gcol[phase, part, :] = jnp.where(lanes == first_expert + idx, column, gcol[phase, part, :])
                picked = jnp.dot(jnp.concatenate(picks, axis=0), tokens_ref[...], preferred_element_type=F32).astype(BF16)
                rows[0, part, :] = picked[:cap]
                rows[1, part, :] = picked[cap:]

        def finish(expert, slot, both):
            act[phase * count + expert, :, slot * col:(slot + 1) * col] = (jax.nn.silu(both[:, :col]) * both[:, col:]).astype(BF16)

        for start in range(0, 2 * wslots, 2):
            for tile in (start, start + 1):
                for copy in w13_copies(first_tile + tile):
                    copy.wait()
            if start == 0:
                gather()
            results = []
            for tile in (start, start + 1):
                idx, slot = divmod(tile, wslots)
                results.append((first_expert + idx, slot,
                                jnp.dot(rows[idx], pool[lax.rem(first_tile + tile, ring)], preferred_element_type=F32)))
            for result in results:
                finish(*result)
            for tile in (start, start + 1):
                ahead = first_tile + tile + ring
                if phase == 0:
                    w13_start(ahead)
                else:
                    @pl.when(ahead < up_tiles)
                    def _(ahead=ahead):
                        w13_start(ahead)

                    @pl.when(ahead >= up_tiles)
                    def _(ahead=ahead):
                        w2_start(ahead - up_tiles)

    gcol[...] = jnp.zeros_like(gcol)
    gate_sends[0].wait_recv()
    pair_send.wait_recv()
    stride = count // 2 // u_chunks

    def near(index, carry):
        up_step(0, index)

        @pl.when(lax.rem(index, stride) == stride - 1)
        def _():
            far_send(index // stride).wait_recv()
            relay_send(index // stride).start()
        return carry
    lax.fori_loop(0, count // 2, near, 0)
    for idx in range(2):
        oh_copy(idx).start()
    gate_sends[1].wait_recv()
    gate_sends[2].wait_recv()
    for idx in range(u_chunks):
        relay_send(idx).wait_recv()

    def away(index, carry):
        up_step(1, index)
        return carry
    lax.fori_loop(0, count // 2, away, 0)

    total_steps = 2 * chunks * groups

    def pair_sum(order):
        slot = lax.rem(order, 2)
        return remote(acc.at[slot, 1], pair_buf.at[slot], ps.at[slot], pr.at[slot], 0)

    def far_sum(chunk):
        return remote(far_src.at[lax.rem(chunk, 3)], far_dst.at[chunk], xs.at[lax.rem(chunk, 3)], xr.at[chunk], 1)

    def mix(step, order, part):
        slot = lax.rem(step, 3)
        for src in range(2):
            hits = jnp.concatenate([oht[slot, src]] * 3, axis=1)
            mixed = jnp.dot(hits, pst[part % 2, src], preferred_element_type=F32)
            if part == 0:
                acc[lax.rem(order, 2), src] = mixed
            else:
                acc[lax.rem(order, 2), src] += mixed

    def settle(order):
        pair_sum(order).wait_recv()
        pair_sum(order).wait_send()
        slot = lax.rem(order, 2)

        @pl.when(order < chunks)
        def _():
            @pl.when(order == 3)
            def _():
                far_sum(0).wait_send()
            far_src[lax.rem(order, 3)] = acc[slot, 0] + pair_buf[slot]
            far_sum(order).start()

        @pl.when(order >= chunks)
        def _():
            chunk = order - chunks
            far_sum(chunk).wait_recv()
            cols = pl.ds(pl.multiple_of(chunk * block, block), block)
            total = acc[slot, 0] + pair_buf[slot]
            out_ref[:, cols] = (hid_ref[:, cols].astype(F32) + total + far_dst[chunk]).astype(BF16)

    def down(order, carry):
        phase = 1 - order // chunks
        for part in range(groups):
            step = order * groups + part
            slot = lax.rem(step + up_tiles, ring)
            for copy in w2_copies(step):
                copy.wait()
            oh_copy(step).wait()
            for idx in range(per):
                expert = part * per + idx
                done = jnp.dot(act[phase * count + expert], pool[slot, idx * width:(idx + 1) * width, :], preferred_element_type=F32).astype(BF16)
                rest = done.astype(F32) * gcol[phase, :, expert:expert + 1]
                for term in range(3):
                    head = rest.astype(BF16)
                    at = (term * per + idx) * cap
                    pst[part % 2, 0, at:at + cap, :] = head[:cap]
                    pst[part % 2, 1, at:at + cap, :] = head[cap:]
                    rest = rest - head.astype(F32)
            if part > 0:
                mix(step - 1, order, part - 1)
            else:
                @pl.when(order > 0)
                def _():
                    mix(step - 1, order - 1, groups - 1)
                    pair_sum(order - 1).start()

            @pl.when(step + ring < total_steps)
            def _():
                w2_start(step + ring)

            @pl.when(step + 2 < total_steps)
            def _():
                oh_copy(step + 2).start()

            if part == 3:
                @pl.when(order > 0)
                def _():
                    settle(order - 1)
        return carry
    lax.fori_loop(0, 2 * chunks, down, 0)
    last = 2 * chunks - 1
    mix(total_steps - 1, last, groups - 1)
    pair_sum(last).start()
    settle(last)

    for send in gate_sends:
        send.wait_send()
    pair_send.wait_send()
    for idx in range(u_chunks):
        far_send(idx).wait_send()
        relay_send(idx).wait_send()
    for idx in range(1, chunks):
        far_sum(idx).wait_send()


def moe(pos_lane, u_own, gates_lane, hidden, w_one, w_three, w_two, onehot, cap):
    seq, model = u_own.shape
    count, _, width = w_one.shape
    u_chunks, chunks, groups, wslots = 4, 4, 8, 4
    block, per = model // chunks, count // groups
    vmem = pl.BlockSpec(memory_space=pltpu.VMEM)
    hbm = pl.BlockSpec(memory_space=pl.ANY)
    dma = pltpu.SemaphoreType.DMA
    return pl.pallas_call(
        functools.partial(moe_kernel, cap=cap, u_chunks=u_chunks, chunks=chunks, groups=groups, wslots=wslots),
        in_specs=[vmem, vmem, vmem, vmem, hbm, hbm, hbm, hbm],
        out_specs=vmem,
        out_shape=jax.ShapeDtypeStruct((seq, model), BF16),
        scratch_shapes=[
            pltpu.VMEM((3, seq, model), BF16), pltpu.VMEM((3, count, seq), F32), pltpu.VMEM((2, 2 * cap, model), BF16),
            pltpu.VMEM((2 * count, 2 * cap, width), BF16), pltpu.VMEM((2, 2 * cap, 128), F32),
            pltpu.VMEM((6, model, block), BF16),
            pltpu.VMEM((3, 2, seq, per * cap), BF16), pltpu.VMEM((2, 2, 3 * per * cap, block), BF16),
            pltpu.VMEM((2, 2, seq, block), F32), pltpu.VMEM((2, seq, block), F32),
            pltpu.VMEM((3, seq, block), F32), pltpu.VMEM((chunks, seq, block), F32),
            dma((1 + 2 * u_chunks,)), dma((1 + 2 * u_chunks,)), dma((3,)), dma((3,)), dma((6, 2)), dma((3,)),
            dma((2,)), dma((2,)), dma((3,)), dma((chunks,))],
        compiler_params=pltpu.CompilerParams(collective_id=1, has_side_effects=True, vmem_limit_bytes=67043328),
        name='moe',
    )(pos_lane, u_own, gates_lane, hidden, w_one, w_three, w_two, onehot)


def solution(mesh):
    tok_spec = P(('dp', 'ep'))
    row_spec = P('ep')

    def local_layer(tokens, w_query, w_key, w_value, w_out, w_router, w_one, w_three, w_two, expert_ids):
        seq, model = tokens.shape[1:]
        head_dim = w_query.shape[2]
        choices = expert_ids.shape[2]
        experts = w_router.shape[1]
        own_experts = w_one.shape[0]
        cap = 2 * seq * choices // experts
        ids = expert_ids[0]
        flat = [w.reshape(w.shape[0], -1) for w in (w_query, w_key, w_value)]
        hidden, u_own, pos, onehot = front(ids.T, tokens[0], *flat, w_out, cap, own_experts, head_dim)
        logits = jnp.dot(rms_norm(hidden), w_router, precision=lax.Precision.HIGHEST, preferred_element_type=F32)
        chosen = jnp.any(ids[:, :, None] == jnp.arange(experts, dtype=jnp.int32), axis=1)
        gates = jax.nn.softmax(jnp.where(chosen, logits, -jnp.inf), axis=-1)
        return moe(pos, u_own, gates.T, hidden, w_one, w_three, w_two, onehot, cap)[None]

    return jax.shard_map(local_layer, mesh=mesh, in_specs=(tok_spec, row_spec, row_spec, row_spec, row_spec, P(), row_spec, row_spec, row_spec, tok_spec), out_specs=tok_spec, check_vma=False)
```

```python
import functools
import jax
import jax.numpy as jnp
from jax import lax
from jax.experimental import pallas as pl
from jax.experimental.pallas import tpu as pltpu
from jax.sharding import PartitionSpec as P

EPS = 1e-6
F32 = jnp.float32
BF16 = jnp.bfloat16


def rms_norm(vals):
    wide = vals.astype(F32)
    return wide * lax.rsqrt(jnp.mean(wide * wide, axis=-1, keepdims=True) + EPS)


def head_attention(q_ref, k_ref, v_ref, out_ref, lanes, rows, scale):
    seq = q_ref.shape[0]
    steps = [slice(start, start + rows) for start in range(0, seq, rows)]
    keep = lax.broadcasted_iota(jnp.int32, (rows, rows), 0) >= lax.broadcasted_iota(jnp.int32, (rows, rows), 1)
    nt_dims = (((1,), (1,)), ((), ()))
    scored = []
    for step in steps:
        tile = q_ref[step, lanes]
        diag = lax.dot_general(tile, k_ref[step, lanes], nt_dims, preferred_element_type=F32)
        parts = [jnp.where(keep, diag, -jnp.inf)]
        if step.start:
            parts.append(lax.dot_general(tile, k_ref[:step.start, lanes], nt_dims, preferred_element_type=F32))
        scored.append(parts)
    weighted = []
    for parts in scored:
        top = functools.reduce(jnp.maximum, [jnp.max(part, axis=-1, keepdims=True) for part in parts])
        expo = [jnp.exp((part - top) * scale) for part in parts]
        total = sum(jnp.sum(part, axis=-1, keepdims=True) for part in expo)
        inverse = 1.0 / total
        weighted.append([(part * inverse).astype(BF16) for part in expo])
    for step, parts in zip(steps, weighted):
        mixed = jnp.dot(parts[0], v_ref[step, lanes], preferred_element_type=F32)
        if step.start:
            mixed += jnp.dot(parts[1], v_ref[:step.start, lanes], preferred_element_type=F32)
        out_ref[step, lanes] = mixed.astype(BF16)


def front_kernel(ids_ref, x_ref, wr_ref, wq_ref, wk_ref, wv_ref, wo_ref, hid_ref, u_ref, pos_ref, gate_ref, oh_ref,
                 full, normed, qkv, ctx, ids_all, oh_buf,
                 own_s, po_s, po_r, xs, xr, ys, yr, rs, rr, ids_s, ids_r, oh_s, *, subs, cap, count, head_dim):
    group, me = lax.axis_index('dp'), lax.axis_index('ep')
    weights = (wq_ref, wk_ref, wv_ref, wo_ref)
    shard, model = wo_ref.shape
    seq = x_ref.shape[0]
    half, cols = shard // 2, model // 2
    order = [(0, 0), (1, 0), (2, 0), (0, 1), (1, 1), (2, 1), (3, 0), (3, 1)]
    heads = model // head_dim

    def remote(src, dst, send, recv, where):
        return pltpu.make_async_remote_copy(src_ref=src, dst_ref=dst, send_sem=send, recv_sem=recv,
                                            device_id=where, device_id_type=pl.DeviceIdType.MESH)

    def block(stage, source, which, sub):
        matrix, side = order[stage]
        rows = half // subs[stage]
        start = pl.multiple_of(source * shard + which * half + sub * rows, rows)
        return full.at[matrix, pl.ds(start, rows), pl.ds(side * cols, cols)]

    def own_rows(matrix):
        return full.at[matrix, pl.ds(pl.multiple_of(me * shard, shard), shard)]

    def own_local(matrix):
        return pltpu.make_async_copy(weights[matrix], own_rows(matrix), own_s.at[matrix])

    def own_pair(matrix):
        return remote(weights[matrix], own_rows(matrix), po_s.at[matrix], po_r.at[matrix], {'ep': me ^ 1})

    def x_copy(stage, sub):
        matrix, side = order[stage]
        rows = half // subs[stage]
        src = weights[matrix].at[pl.ds(pl.multiple_of(group * half + sub * rows, rows), rows), pl.ds(side * cols, cols)]
        sem = sum(subs[:stage]) + sub
        return remote(src, block(stage, me, group, sub), xs.at[sem], xr.at[sem], {'ep': me ^ 2})

    def y_copy(stage, sub):
        ref = block(stage, me ^ 2, group, sub)
        sem = sum(subs[:stage]) + sub
        return remote(ref, ref, ys.at[sem], yr.at[sem], {'dp': 1 - group})

    def relay(stage, sub, other):
        ref = block(stage, me ^ 2, 1 - group if other else group, sub)
        sem = (sum(subs[:stage]) + sub) * 2 + other
        return remote(ref, ref, rs.at[sem], rr.at[sem], {'ep': me ^ 1})

    def ids_copy(relation):
        return remote(ids_ref, ids_all.at[relation - 1], ids_s.at[relation - 1], ids_r.at[relation - 1], {'ep': me ^ relation})

    def oh_copy(source):
        return pltpu.make_async_copy(oh_buf.at[source % 2], oh_ref.at[source], oh_s.at[source % 2])

    barrier = pltpu.get_barrier_semaphore()
    for peer in ({'ep': me ^ 1}, {'ep': me ^ 2}, {'ep': me ^ 3}, {'dp': 1 - group}):
        pl.semaphore_signal(barrier, inc=1, device_id=peer, device_id_type=pl.DeviceIdType.MESH)
    pl.semaphore_wait(barrier, 4)

    for relation in (1, 2, 3):
        ids_copy(relation).start()
    messages = [(stage, sub) for stage in range(len(order)) for sub in range(subs[stage])]
    for message in messages:
        x_copy(*message).start()
    for matrix in range(4):
        own_pair(matrix).start()
        own_local(matrix).start()

    normed[...] = rms_norm(x_ref[...]).astype(BF16)

    def place_tokens():
        for relation in (1, 2, 3):
            ids_copy(relation).wait_recv()
        mine = lax.broadcasted_iota(jnp.int32, (count, seq), 0) + me * count
        earlier = (lax.broadcasted_iota(jnp.int32, (seq, seq), 0) < lax.broadcasted_iota(jnp.int32, (seq, seq), 1))
        earlier = earlier.astype(F32).astype(BF16)
        places = []
        for source in range(4):
            ids = ids_ref[...] if source == 0 else ids_all[source - 1]
            member = mine == ids[0:1, :]
            for choice in range(1, ids.shape[0]):
                member = jnp.logical_or(member, mine == ids[choice:choice + 1, :])
            before = jnp.dot(member.astype(F32).astype(BF16), earlier, preferred_element_type=F32)
            places.append(jnp.where(member, before, -1.0))
            pos_ref[source] = places[source].astype(jnp.int32)
        filler = jnp.zeros((128 - 4 * count, seq), F32)
        by_token = jnp.concatenate(places + [filler], axis=0).T
        slots = lax.broadcasted_iota(jnp.int32, (seq, cap), 1).astype(F32)
        for source in range(4):
            if source >= 2:
                oh_copy(source - 2).wait()
            for expert in range(count):
                lane = source * count + expert
                hit = by_token[:, lane:lane + 1] == slots
                oh_buf[source % 2, :, expert * cap:(expert + 1) * cap] = hit.astype(F32).astype(BF16)
            oh_copy(source).start()

    def ready(stage):
        matrix, side = order[stage]
        if side == 0:
            own_local(matrix).wait()
            own_pair(matrix).wait_recv()
        for sub in range(subs[stage]):
            relay(stage, sub, 0).wait_recv()
            relay(stage, sub, 1).wait_recv()

    def project(stage):
        matrix, side = order[stage]

        def body(idx, carry):
            lanes = pl.ds(pl.multiple_of(side * cols + idx * 256, 256), 256)
            qkv[matrix, :, lanes] = jnp.dot(normed[...], full[matrix, :, lanes], preferred_element_type=F32).astype(BF16)
            return carry
        lax.fori_loop(0, cols // 256, body, 0)

    def attend(first, last):
        def body(head, carry):
            lanes = pl.ds(pl.multiple_of(head * head_dim, head_dim), head_dim)
            head_attention(qkv.at[0], qkv.at[1], qkv.at[2], ctx, lanes, 128, head_dim ** -0.5)
            return carry
        lax.fori_loop(first, last, body, 0)

    def combine(stage):
        side = order[stage][1]

        def body(idx, carry):
            lanes = pl.ds(pl.multiple_of(side * cols + idx * 256, 256), 256)
            mixed = jnp.dot(ctx[...], full[3, :, lanes], preferred_element_type=F32)
            hid_ref[:, lanes] = (x_ref[:, lanes].astype(F32) + mixed).astype(BF16)
            return carry
        lax.fori_loop(0, cols // 256, body, 0)

    def work(stage, sub):
        if sub == 0 and stage > 0:
            ready(stage - 1)
            if stage - 1 < 6:
                project(stage - 1)
            if stage - 1 == 6:
                attend(heads - 2, heads)
                combine(6)
        if sub == 0 and stage in (3, 4):
            attend((stage - 3) * heads // 4, (stage - 2) * heads // 4)
        if sub == 0 and stage == 6:
            attend(heads // 2, heads - 2)

    place_tokens()
    previous = None
    for message in messages:
        x_copy(*message).wait_recv()
        y_copy(*message).start()
        relay(*message, 0).start()
        if previous is not None:
            y_copy(*previous).wait_recv()
            relay(*previous, 1).start()
        work(*message)
        previous = message
    y_copy(*previous).wait_recv()
    relay(*previous, 1).start()
    ready(7)
    combine(7)
    wide = hid_ref[...].astype(F32)
    scale = lax.rsqrt(jnp.mean(wide * wide, axis=-1, keepdims=True) + EPS)
    experts = wr_ref.shape[0]
    logits = jnp.zeros((experts, seq), F32)
    for start in range(0, model, 512):
        lanes = slice(start, start + 512)
        state = hid_ref[:, lanes].astype(F32) * scale
        u_ref[:, lanes] = state.astype(BF16)
        logits += lax.dot_general(wr_ref[:, lanes], state, (((1,), (1,)), ((), ())),
                                  precision=lax.Precision.HIGHEST, preferred_element_type=F32)
    ids = ids_ref[...]
    numbers = lax.broadcasted_iota(jnp.int32, (experts, seq), 0)
    chosen = numbers == ids[0:1, :]
    for choice in range(1, ids.shape[0]):
        chosen = jnp.logical_or(chosen, numbers == ids[choice:choice + 1, :])
    logits = jnp.where(chosen, logits, -jnp.inf)
    expo = jnp.exp(logits - jnp.max(logits, axis=0, keepdims=True))
    gate_ref[...] = expo / jnp.sum(expo, axis=0, keepdims=True)

    oh_copy(2).wait()
    oh_copy(3).wait()
    for relation in (1, 2, 3):
        ids_copy(relation).wait_send()
    for matrix in range(4):
        own_pair(matrix).wait_send()
    for message in messages:
        x_copy(*message).wait_send()
        y_copy(*message).wait_send()
        relay(*message, 0).wait_send()
        relay(*message, 1).wait_send()


def front(ids_lane, tokens, router_lane, w_query, w_key, w_value, w_out, cap, count, head_dim):
    seq, model = tokens.shape
    subs = (1, 1, 1, 1, 1, 1, 1, 2)
    vmem = pl.BlockSpec(memory_space=pltpu.VMEM)
    hbm = pl.BlockSpec(memory_space=pl.ANY)
    dma = pltpu.SemaphoreType.DMA
    sends = sum(subs)
    return pl.pallas_call(
        functools.partial(front_kernel, subs=subs, cap=cap, count=count, head_dim=head_dim),
        in_specs=[vmem, vmem, vmem, hbm, hbm, hbm, hbm],
        out_specs=[vmem, vmem, vmem, vmem, hbm],
        out_shape=[jax.ShapeDtypeStruct((seq, model), BF16), jax.ShapeDtypeStruct((seq, model), BF16),
                   jax.ShapeDtypeStruct((4, count, seq), jnp.int32),
                   jax.ShapeDtypeStruct((router_lane.shape[0], seq), F32), jax.ShapeDtypeStruct((4, seq, count * cap), BF16)],
        scratch_shapes=[
            pltpu.VMEM((4, model, model), BF16), pltpu.VMEM((seq, model), BF16), pltpu.VMEM((3, seq, model), BF16),
            pltpu.VMEM((seq, model), BF16), pltpu.VMEM((3,) + ids_lane.shape, jnp.int32), pltpu.VMEM((2, seq, count * cap), BF16),
            dma((4,)), dma((4,)), dma((4,)), dma((sends,)), dma((sends,)), dma((sends,)), dma((sends,)),
            dma((2 * sends,)), dma((2 * sends,)), dma((3,)), dma((3,)), dma((2,))],
        compiler_params=pltpu.CompilerParams(collective_id=2, has_side_effects=True, vmem_limit_bytes=67043328),
        name='front',
    )(ids_lane, tokens, router_lane, w_query, w_key, w_value, w_out)


def moe_kernel(pos_ref, u_ref, gate_ref, hid_ref, w1_ref, w3_ref, w2_ref, oh_ref, out_ref,
               ug, gg, rows, act, gcol, pool, oht, pst, acc, pair_buf, far_src, far_dst,
               us, ur, gs, gr, ws, ohs, ps, pr, xs, xr,
               *, cap, u_chunks, chunks, groups, wslots):
    me = lax.axis_index('ep')
    relations = (me ^ 1, me ^ 2, me ^ 3)
    seq, model = u_ref.shape
    count, _, width = w1_ref.shape
    col = width // wslots
    block = model // chunks
    per = count // groups
    piece = seq // u_chunks

    def remote(src, dst, send, recv, relation):
        return pltpu.make_async_remote_copy(src_ref=src, dst_ref=dst, send_sem=send, recv_sem=recv,
                                            device_id={'ep': relations[relation]}, device_id_type=pl.DeviceIdType.MESH)

    ring = pool.shape[0]
    up_tiles = 2 * count * wslots

    def w13_copies(tile):
        slot, expert = lax.rem(tile, ring), lax.rem(tile // wslots, count)
        at = pl.multiple_of(lax.rem(tile, wslots) * col, col)
        return [pltpu.make_async_copy(ref.at[expert, :, pl.ds(at, col)], pool.at[slot, :, pl.ds(which * col, col)], ws.at[slot, which])
                for which, ref in enumerate((w1_ref, w3_ref))]

    def w2_copies(step):
        slot = lax.rem(step + up_tiles, ring)
        at = pl.multiple_of(lax.rem(step // groups, chunks) * block, block)
        return [pltpu.make_async_copy(w2_ref.at[lax.rem(step, groups) * per + idx, :, pl.ds(at, block)],
                                      pool.at[slot, pl.ds(idx * width, width), :], ws.at[slot, idx]) for idx in range(per)]

    def w13_start(tile):
        for copy in w13_copies(tile):
            copy.start()

    def w2_start(step):
        for copy in w2_copies(step):
            copy.start()

    def oh_copy(step):
        slot = lax.rem(step, 3)
        phase = 1 - step // (groups * chunks)
        depth = per * cap
        return pltpu.make_async_copy(oh_ref.at[pl.ds(2 * phase, 2), :,
                                               pl.ds(pl.multiple_of(lax.rem(step, groups) * depth, depth), depth)],
                                     oht.at[slot], ohs.at[slot])

    for tile in range(ring):
        w13_start(tile)

    barrier = pltpu.get_barrier_semaphore()
    for peer in relations:
        pl.semaphore_signal(barrier, inc=1, device_id={'ep': peer}, device_id_type=pl.DeviceIdType.MESH)
    pl.semaphore_wait(barrier, 3)

    gate_sends = [remote(gate_ref.at[pl.ds(pl.multiple_of(relations[r] * count, count), count)], gg.at[r], gs.at[r], gr.at[r], r)
                  for r in range(3)]
    pair_send = remote(u_ref, ug.at[0], us.at[0], ur.at[0], 0)

    def far_send(idx):
        part = pl.ds(pl.multiple_of(idx * piece, piece), piece)
        return remote(u_ref.at[part], ug.at[1, part], us.at[1 + idx], ur.at[1 + idx], 1)

    def relay_send(idx):
        part = pl.ds(pl.multiple_of(idx * piece, piece), piece)
        return remote(ug.at[1, part], ug.at[2, part], us.at[1 + u_chunks + idx], ur.at[1 + u_chunks + idx], 0)

    for send in gate_sends:
        send.start()
    for idx in range(u_chunks):
        far_send(idx).start()
    pair_send.start()

    slots = lax.broadcasted_iota(jnp.int32, (cap, seq), 0)
    lanes = lax.broadcasted_iota(jnp.int32, (cap, 128), 1)

    def up_step(phase, index):
        first_expert = 2 * index
        first_tile = (phase * count + first_expert) * wslots
        if phase == 0:
            sources = ((u_ref, gate_ref, me * count), (ug.at[0], gg.at[0], 0))
        else:
            sources = ((ug.at[1], gg.at[1], 0), (ug.at[2], gg.at[2], 0))

        def gather():
            for src, (tokens_ref, gates_ref, offset) in enumerate(sources):
                part = slice(src * cap, (src + 1) * cap)
                picks = []
                for idx in range(2):
                    hit = pos_ref[2 * phase + src, pl.ds(first_expert + idx, 1), :] == slots
                    picks.append(hit.astype(F32).astype(BF16))
                    gate_row = gates_ref[pl.ds(offset + first_expert + idx, 1), :]
                    column = jnp.sum(jnp.where(hit, gate_row, 0.0), axis=-1, keepdims=True)
                    gcol[phase, part, :] = jnp.where(lanes == first_expert + idx, column, gcol[phase, part, :])
                picked = jnp.dot(jnp.concatenate(picks, axis=0), tokens_ref[...], preferred_element_type=F32).astype(BF16)
                rows[0, part, :] = picked[:cap]
                rows[1, part, :] = picked[cap:]

        def finish(expert, slot, both):
            act[phase * count + expert, :, slot * col:(slot + 1) * col] = (jax.nn.silu(both[:, :col]) * both[:, col:]).astype(BF16)

        for start in range(0, 2 * wslots, 2):
            for tile in (start, start + 1):
                for copy in w13_copies(first_tile + tile):
                    copy.wait()
            if start == 0:
                gather()
            results = []
            for tile in (start, start + 1):
                idx, slot = divmod(tile, wslots)
                results.append((first_expert + idx, slot,
                                jnp.dot(rows[idx], pool[lax.rem(first_tile + tile, ring)], preferred_element_type=F32)))
            for result in results:
                finish(*result)
            for tile in (start, start + 1):
                ahead = first_tile + tile + ring
                if phase == 0:
                    w13_start(ahead)
                else:
                    @pl.when(ahead < up_tiles)
                    def _(ahead=ahead):
                        w13_start(ahead)

                    @pl.when(ahead >= up_tiles)
                    def _(ahead=ahead):
                        w2_start(ahead - up_tiles)

    gcol[...] = jnp.zeros_like(gcol)
    gate_sends[0].wait_recv()
    pair_send.wait_recv()
    stride = count // 2 // u_chunks

    def near(index, carry):
        up_step(0, index)

        @pl.when(lax.rem(index, stride) == stride - 1)
        def _():
            far_send(index // stride).wait_recv()
            relay_send(index // stride).start()
        return carry
    lax.fori_loop(0, count // 2, near, 0)
    for idx in range(2):
        oh_copy(idx).start()
    gate_sends[1].wait_recv()
    gate_sends[2].wait_recv()
    for idx in range(u_chunks):
        relay_send(idx).wait_recv()

    def away(index, carry):
        up_step(1, index)
        return carry
    lax.fori_loop(0, count // 2, away, 0)

    total_steps = 2 * chunks * groups

    def pair_sum(order):
        slot = lax.rem(order, 2)
        return remote(acc.at[slot, 1], pair_buf.at[slot], ps.at[slot], pr.at[slot], 0)

    def far_sum(chunk):
        return remote(far_src.at[lax.rem(chunk, 3)], far_dst.at[chunk], xs.at[lax.rem(chunk, 3)], xr.at[chunk], 1)

    def mix(step, order, part):
        slot = lax.rem(step, 3)
        for src in range(2):
            hits = jnp.concatenate([oht[slot, src]] * 3, axis=1)
            mixed = jnp.dot(hits, pst[part % 2, src], preferred_element_type=F32)
            if part == 0:
                acc[lax.rem(order, 2), src] = mixed
            else:
                acc[lax.rem(order, 2), src] += mixed

    def settle(order):
        pair_sum(order).wait_recv()
        pair_sum(order).wait_send()
        slot = lax.rem(order, 2)

        @pl.when(order < chunks)
        def _():
            @pl.when(order == 3)
            def _():
                far_sum(0).wait_send()
            far_src[lax.rem(order, 3)] = acc[slot, 0] + pair_buf[slot]
            far_sum(order).start()

        @pl.when(order >= chunks)
        def _():
            chunk = order - chunks
            far_sum(chunk).wait_recv()
            cols = pl.ds(pl.multiple_of(chunk * block, block), block)
            total = acc[slot, 0] + pair_buf[slot]
            out_ref[:, cols] = (hid_ref[:, cols].astype(F32) + total + far_dst[chunk]).astype(BF16)

    def down(order, carry):
        phase = 1 - order // chunks
        for part in range(groups):
            step = order * groups + part
            slot = lax.rem(step + up_tiles, ring)
            for copy in w2_copies(step):
                copy.wait()
            oh_copy(step).wait()
            for idx in range(per):
                expert = part * per + idx
                done = jnp.dot(act[phase * count + expert], pool[slot, idx * width:(idx + 1) * width, :], preferred_element_type=F32).astype(BF16)
                rest = done.astype(F32) * gcol[phase, :, expert:expert + 1]
                for term in range(3):
                    head = rest.astype(BF16)
                    at = (term * per + idx) * cap
                    pst[part % 2, 0, at:at + cap, :] = head[:cap]
                    pst[part % 2, 1, at:at + cap, :] = head[cap:]
                    rest = rest - head.astype(F32)
            if part > 0:
                mix(step - 1, order, part - 1)
            else:
                @pl.when(order > 0)
                def _():
                    mix(step - 1, order - 1, groups - 1)
                    pair_sum(order - 1).start()

            @pl.when(step + ring < total_steps)
            def _():
                w2_start(step + ring)

            @pl.when(step + 2 < total_steps)
            def _():
                oh_copy(step + 2).start()

            if part == 3:
                @pl.when(order > 0)
                def _():
                    settle(order - 1)
        return carry
    lax.fori_loop(0, 2 * chunks, down, 0)
    last = 2 * chunks - 1
    mix(total_steps - 1, last, groups - 1)
    pair_sum(last).start()
    settle(last)

    for send in gate_sends:
        send.wait_send()
    pair_send.wait_send()
    for idx in range(u_chunks):
        far_send(idx).wait_send()
        relay_send(idx).wait_send()
    for idx in range(1, chunks):
        far_sum(idx).wait_send()


def moe(pos_lane, u_own, gates_lane, hidden, w_one, w_three, w_two, onehot, cap):
    seq, model = u_own.shape
    count, _, width = w_one.shape
    u_chunks, chunks, groups, wslots = 4, 4, 8, 4
    block, per = model // chunks, count // groups
    vmem = pl.BlockSpec(memory_space=pltpu.VMEM)
    hbm = pl.BlockSpec(memory_space=pl.ANY)
    dma = pltpu.SemaphoreType.DMA
    return pl.pallas_call(
        functools.partial(moe_kernel, cap=cap, u_chunks=u_chunks, chunks=chunks, groups=groups, wslots=wslots),
        in_specs=[vmem, vmem, vmem, vmem, hbm, hbm, hbm, hbm],
        out_specs=vmem,
        out_shape=jax.ShapeDtypeStruct((seq, model), BF16),
        scratch_shapes=[
            pltpu.VMEM((3, seq, model), BF16), pltpu.VMEM((3, count, seq), F32), pltpu.VMEM((2, 2 * cap, model), BF16),
            pltpu.VMEM((2 * count, 2 * cap, width), BF16), pltpu.VMEM((2, 2 * cap, 128), F32),
            pltpu.VMEM((6, model, block), BF16),
            pltpu.VMEM((3, 2, seq, per * cap), BF16), pltpu.VMEM((2, 2, 3 * per * cap, block), BF16),
            pltpu.VMEM((2, 2, seq, block), F32), pltpu.VMEM((2, seq, block), F32),
            pltpu.VMEM((3, seq, block), F32), pltpu.VMEM((chunks, seq, block), F32),
            dma((1 + 2 * u_chunks,)), dma((1 + 2 * u_chunks,)), dma((3,)), dma((3,)), dma((6, 2)), dma((3,)),
            dma((2,)), dma((2,)), dma((3,)), dma((chunks,))],
        compiler_params=pltpu.CompilerParams(collective_id=1, has_side_effects=True, vmem_limit_bytes=67043328),
        name='moe',
    )(pos_lane, u_own, gates_lane, hidden, w_one, w_three, w_two, onehot)


def solution(mesh):
    tok_spec = P(('dp', 'ep'))
    row_spec = P('ep')

    def local_layer(tokens, w_query, w_key, w_value, w_out, w_router, w_one, w_three, w_two, expert_ids):
        seq, model = tokens.shape[1:]
        head_dim = w_query.shape[2]
        choices = expert_ids.shape[2]
        experts = w_router.shape[1]
        own_experts = w_one.shape[0]
        cap = 2 * seq * choices // experts
        ids = expert_ids[0]
        flat = [w.reshape(w.shape[0], -1) for w in (w_query, w_key, w_value)]
        hidden, u_own, pos, gates, onehot = front(ids.T, tokens[0], w_router.T, *flat, w_out, cap, own_experts, head_dim)
        return moe(pos, u_own, gates, hidden, w_one, w_three, w_two, onehot, cap)[None]

    return jax.shard_map(local_layer, mesh=mesh, in_specs=(tok_spec, row_spec, row_spec, row_spec, row_spec, P(), row_spec, row_spec, row_spec, tok_spec), out_specs=tok_spec, check_vma=False)
```

```python
import functools
import jax
import jax.numpy as jnp
from jax import lax
from jax.experimental import pallas as pl
from jax.experimental.pallas import tpu as pltpu
from jax.sharding import PartitionSpec as P

EPS = 1e-6
F32 = jnp.float32
BF16 = jnp.bfloat16


def rms_norm(vals):
    wide = vals.astype(F32)
    return wide * lax.rsqrt(jnp.mean(wide * wide, axis=-1, keepdims=True) + EPS)


def head_attention(q_ref, k_ref, v_ref, out_ref, lanes, rows, scale):
    seq = q_ref.shape[0]
    steps = [slice(start, start + rows) for start in range(0, seq, rows)]
    keep = lax.broadcasted_iota(jnp.int32, (rows, rows), 0) >= lax.broadcasted_iota(jnp.int32, (rows, rows), 1)
    nt_dims = (((1,), (1,)), ((), ()))
    scored = []
    for step in steps:
        tile = q_ref[step, lanes]
        diag = lax.dot_general(tile, k_ref[step, lanes], nt_dims, preferred_element_type=F32)
        parts = [jnp.where(keep, diag, -jnp.inf)]
        if step.start:
            parts.append(lax.dot_general(tile, k_ref[:step.start, lanes], nt_dims, preferred_element_type=F32))
        scored.append(parts)
    weighted = []
    for parts in scored:
        top = functools.reduce(jnp.maximum, [jnp.max(part, axis=-1, keepdims=True) for part in parts])
        expo = [jnp.exp((part - top) * scale) for part in parts]
        total = sum(jnp.sum(part, axis=-1, keepdims=True) for part in expo)
        inverse = 1.0 / total
        weighted.append([(part * inverse).astype(BF16) for part in expo])
    for step, parts in zip(steps, weighted):
        mixed = jnp.dot(parts[0], v_ref[step, lanes], preferred_element_type=F32)
        if step.start:
            mixed += jnp.dot(parts[1], v_ref[:step.start, lanes], preferred_element_type=F32)
        out_ref[step, lanes] = mixed.astype(BF16)


def front_kernel(ids_ref, x_ref, wr_ref, wq_ref, wk_ref, wv_ref, wo_ref, hid_ref, u_ref, pos_ref, gate_ref, oh_ref,
                 full, normed, qkv, ctx, ids_all, oh_buf,
                 own_s, po_s, po_r, xs, xr, ys, yr, rs, rr, ids_s, ids_r, oh_s, *, subs, cap, count, head_dim):
    group, me = lax.axis_index('dp'), lax.axis_index('ep')
    weights = (wq_ref, wk_ref, wv_ref, wo_ref)
    shard, model = wo_ref.shape
    seq = x_ref.shape[0]
    half, cols = shard // 2, model // 2
    order = [(0, 0), (1, 0), (2, 0), (0, 1), (1, 1), (2, 1), (3, 0), (3, 1)]
    heads = model // head_dim

    def remote(src, dst, send, recv, where):
        return pltpu.make_async_remote_copy(src_ref=src, dst_ref=dst, send_sem=send, recv_sem=recv,
                                            device_id=where, device_id_type=pl.DeviceIdType.MESH)

    def block(stage, source, which, sub):
        matrix, side = order[stage]
        rows = half // subs[stage]
        start = pl.multiple_of(source * shard + which * half + sub * rows, rows)
        return full.at[matrix, pl.ds(start, rows), pl.ds(side * cols, cols)]

    def own_rows(matrix):
        return full.at[matrix, pl.ds(pl.multiple_of(me * shard, shard), shard)]

    def own_local(matrix):
        return pltpu.make_async_copy(weights[matrix], own_rows(matrix), own_s.at[matrix])

    def own_pair(matrix):
        return remote(weights[matrix], own_rows(matrix), po_s.at[matrix], po_r.at[matrix], {'ep': me ^ 1})

    def x_copy(stage, sub):
        matrix, side = order[stage]
        rows = half // subs[stage]
        src = weights[matrix].at[pl.ds(pl.multiple_of(group * half + sub * rows, rows), rows), pl.ds(side * cols, cols)]
        sem = sum(subs[:stage]) + sub
        return remote(src, block(stage, me, group, sub), xs.at[sem], xr.at[sem], {'ep': me ^ 2})

    def y_copy(stage, sub):
        ref = block(stage, me ^ 2, group, sub)
        sem = sum(subs[:stage]) + sub
        return remote(ref, ref, ys.at[sem], yr.at[sem], {'dp': 1 - group})

    def relay(stage, sub, other):
        ref = block(stage, me ^ 2, 1 - group if other else group, sub)
        sem = (sum(subs[:stage]) + sub) * 2 + other
        return remote(ref, ref, rs.at[sem], rr.at[sem], {'ep': me ^ 1})

    def ids_copy(relation):
        return remote(ids_ref, ids_all.at[relation - 1], ids_s.at[relation - 1], ids_r.at[relation - 1], {'ep': me ^ relation})

    def oh_copy(source):
        return pltpu.make_async_copy(oh_buf.at[source % 2], oh_ref.at[source], oh_s.at[source % 2])

    barrier = pltpu.get_barrier_semaphore()
    for peer in ({'ep': me ^ 1}, {'ep': me ^ 2}, {'ep': me ^ 3}, {'dp': 1 - group}):
        pl.semaphore_signal(barrier, inc=1, device_id=peer, device_id_type=pl.DeviceIdType.MESH)
    pl.semaphore_wait(barrier, 4)

    for relation in (1, 2, 3):
        ids_copy(relation).start()
    messages = [(stage, sub) for stage in range(len(order)) for sub in range(subs[stage])]
    for message in messages:
        x_copy(*message).start()
    for matrix in range(4):
        own_pair(matrix).start()
        own_local(matrix).start()

    normed[...] = rms_norm(x_ref[...]).astype(BF16)

    def place_tokens():
        for relation in (1, 2, 3):
            ids_copy(relation).wait_recv()
        mine = lax.broadcasted_iota(jnp.int32, (count, seq), 0) + me * count
        earlier = (lax.broadcasted_iota(jnp.int32, (seq, seq), 0) < lax.broadcasted_iota(jnp.int32, (seq, seq), 1))
        earlier = earlier.astype(F32).astype(BF16)
        places = []
        for source in range(4):
            ids = ids_ref[...] if source == 0 else ids_all[source - 1]
            member = mine == ids[0:1, :]
            for choice in range(1, ids.shape[0]):
                member = jnp.logical_or(member, mine == ids[choice:choice + 1, :])
            before = jnp.dot(member.astype(F32).astype(BF16), earlier, preferred_element_type=F32)
            places.append(jnp.where(member, before, -1.0))
            pos_ref[source] = places[source].astype(jnp.int32)
        filler = jnp.zeros((128 - 4 * count, seq), F32)
        by_token = jnp.concatenate(places + [filler], axis=0).T
        slots = lax.broadcasted_iota(jnp.int32, (seq, cap), 1).astype(F32)
        for source in range(4):
            if source >= 2:
                oh_copy(source - 2).wait()
            for expert in range(count):
                lane = source * count + expert
                hit = by_token[:, lane:lane + 1] == slots
                oh_buf[source % 2, :, expert * cap:(expert + 1) * cap] = hit.astype(F32).astype(BF16)
            oh_copy(source).start()

    def ready(stage):
        matrix, side = order[stage]
        if side == 0:
            own_local(matrix).wait()
            own_pair(matrix).wait_recv()
        for sub in range(subs[stage]):
            relay(stage, sub, 0).wait_recv()
            relay(stage, sub, 1).wait_recv()

    def project(stage):
        matrix, side = order[stage]

        def body(idx, carry):
            lanes = pl.ds(pl.multiple_of(side * cols + idx * 256, 256), 256)
            qkv[matrix, :, lanes] = jnp.dot(normed[...], full[matrix, :, lanes], preferred_element_type=F32).astype(BF16)
            return carry
        lax.fori_loop(0, cols // 256, body, 0)

    def attend(first, last):
        def body(head, carry):
            lanes = pl.ds(pl.multiple_of(head * head_dim, head_dim), head_dim)
            head_attention(qkv.at[0], qkv.at[1], qkv.at[2], ctx, lanes, 128, head_dim ** -0.5)
            return carry
        lax.fori_loop(first, last, body, 0)

    def combine(stage):
        side = order[stage][1]

        def body(idx, carry):
            lanes = pl.ds(pl.multiple_of(side * cols + idx * 256, 256), 256)
            mixed = jnp.dot(ctx[...], full[3, :, lanes], preferred_element_type=F32)
            hid_ref[:, lanes] = (x_ref[:, lanes].astype(F32) + mixed).astype(BF16)
            return carry
        lax.fori_loop(0, cols // 256, body, 0)

    def work(stage, sub):
        if sub == 0 and stage > 0:
            ready(stage - 1)
            if stage - 1 < 6:
                project(stage - 1)
            if stage - 1 == 6:
                attend(heads - 2, heads)
                combine(6)
        if sub == 0 and stage in (3, 4):
            attend((stage - 3) * heads // 4, (stage - 2) * heads // 4)
        if sub == 0 and stage == 6:
            attend(heads // 2, heads - 2)

    place_tokens()
    previous = None
    for message in messages:
        x_copy(*message).wait_recv()
        y_copy(*message).start()
        relay(*message, 0).start()
        if previous is not None:
            y_copy(*previous).wait_recv()
            relay(*previous, 1).start()
        work(*message)
        previous = message
    y_copy(*previous).wait_recv()
    relay(*previous, 1).start()
    ready(7)
    combine(7)
    wide = hid_ref[...].astype(F32)
    scale = lax.rsqrt(jnp.mean(wide * wide, axis=-1, keepdims=True) + EPS)
    experts = wr_ref.shape[0]
    logits = jnp.zeros((experts, seq), F32)
    for start in range(0, model, 512):
        lanes = slice(start, start + 512)
        state = hid_ref[:, lanes].astype(F32) * scale
        u_ref[:, lanes] = state.astype(BF16)
        logits += lax.dot_general(wr_ref[:, lanes], state, (((1,), (1,)), ((), ())),
                                  precision=lax.Precision.HIGHEST, preferred_element_type=F32)
    ids = ids_ref[...]
    numbers = lax.broadcasted_iota(jnp.int32, (experts, seq), 0)
    chosen = numbers == ids[0:1, :]
    for choice in range(1, ids.shape[0]):
        chosen = jnp.logical_or(chosen, numbers == ids[choice:choice + 1, :])
    logits = jnp.where(chosen, logits, -jnp.inf)
    expo = jnp.exp(logits - jnp.max(logits, axis=0, keepdims=True))
    gate_ref[...] = expo / jnp.sum(expo, axis=0, keepdims=True)

    oh_copy(2).wait()
    oh_copy(3).wait()
    for relation in (1, 2, 3):
        ids_copy(relation).wait_send()
    for matrix in range(4):
        own_pair(matrix).wait_send()
    for message in messages:
        x_copy(*message).wait_send()
        y_copy(*message).wait_send()
        relay(*message, 0).wait_send()
        relay(*message, 1).wait_send()


def front(ids_lane, tokens, router_lane, w_query, w_key, w_value, w_out, cap, count, head_dim):
    seq, model = tokens.shape
    subs = (1, 1, 1, 1, 1, 1, 1, 2)
    vmem = pl.BlockSpec(memory_space=pltpu.VMEM)
    hbm = pl.BlockSpec(memory_space=pl.ANY)
    dma = pltpu.SemaphoreType.DMA
    sends = sum(subs)
    return pl.pallas_call(
        functools.partial(front_kernel, subs=subs, cap=cap, count=count, head_dim=head_dim),
        in_specs=[vmem, vmem, vmem, hbm, hbm, hbm, hbm],
        out_specs=[vmem, vmem, vmem, vmem, hbm],
        out_shape=[jax.ShapeDtypeStruct((seq, model), BF16), jax.ShapeDtypeStruct((seq, model), BF16),
                   jax.ShapeDtypeStruct((4, count, seq), jnp.int32),
                   jax.ShapeDtypeStruct((router_lane.shape[0], seq), F32), jax.ShapeDtypeStruct((4, seq, count * cap), BF16)],
        scratch_shapes=[
            pltpu.VMEM((4, model, model), BF16), pltpu.VMEM((seq, model), BF16), pltpu.VMEM((3, seq, model), BF16),
            pltpu.VMEM((seq, model), BF16), pltpu.VMEM((3,) + ids_lane.shape, jnp.int32), pltpu.VMEM((2, seq, count * cap), BF16),
            dma((4,)), dma((4,)), dma((4,)), dma((sends,)), dma((sends,)), dma((sends,)), dma((sends,)),
            dma((2 * sends,)), dma((2 * sends,)), dma((3,)), dma((3,)), dma((2,))],
        compiler_params=pltpu.CompilerParams(collective_id=2, has_side_effects=True, vmem_limit_bytes=67043328),
        name='front',
    )(ids_lane, tokens, router_lane, w_query, w_key, w_value, w_out)


def moe_kernel(pos_ref, u_ref, gate_ref, hid_ref, w1_ref, w3_ref, w2_ref, oh_ref, out_ref,
               ug, gg, rows, raw, act, gcol, pool, oht, pst, acc, pair_buf, far_src, far_dst,
               us, ur, gs, gr, ws, ohs, ps, pr, xs, xr,
               *, cap, u_chunks, chunks, groups, wslots):
    me = lax.axis_index('ep')
    relations = (me ^ 1, me ^ 2, me ^ 3)
    seq, model = u_ref.shape
    count, _, width = w1_ref.shape
    col = width // wslots
    block = model // chunks
    per = count // groups
    piece = seq // u_chunks

    def remote(src, dst, send, recv, relation):
        return pltpu.make_async_remote_copy(src_ref=src, dst_ref=dst, send_sem=send, recv_sem=recv,
                                            device_id={'ep': relations[relation]}, device_id_type=pl.DeviceIdType.MESH)

    ring = pool.shape[0]
    up_tiles = 2 * count * wslots

    def w13_copies(tile):
        slot, expert = lax.rem(tile, ring), lax.rem(tile // wslots, count)
        at = pl.multiple_of(lax.rem(tile, wslots) * col, col)
        return [pltpu.make_async_copy(ref.at[expert, :, pl.ds(at, col)], pool.at[slot, :, pl.ds(which * col, col)], ws.at[slot, which])
                for which, ref in enumerate((w1_ref, w3_ref))]

    def w2_copies(step):
        slot = lax.rem(step + up_tiles, ring)
        at = pl.multiple_of(lax.rem(step // groups, chunks) * block, block)
        return [pltpu.make_async_copy(w2_ref.at[lax.rem(step, groups) * per + idx, :, pl.ds(at, block)],
                                      pool.at[slot, pl.ds(idx * width, width), :], ws.at[slot, idx]) for idx in range(per)]

    def w13_start(tile):
        for copy in w13_copies(tile):
            copy.start()

    def w2_start(step):
        for copy in w2_copies(step):
            copy.start()

    def oh_copy(step):
        slot = lax.rem(step, 3)
        phase = 1 - step // (groups * chunks)
        depth = per * cap
        return pltpu.make_async_copy(oh_ref.at[pl.ds(2 * phase, 2), :,
                                               pl.ds(pl.multiple_of(lax.rem(step, groups) * depth, depth), depth)],
                                     oht.at[slot], ohs.at[slot])

    for tile in range(ring):
        w13_start(tile)

    barrier = pltpu.get_barrier_semaphore()
    for peer in relations:
        pl.semaphore_signal(barrier, inc=1, device_id={'ep': peer}, device_id_type=pl.DeviceIdType.MESH)
    pl.semaphore_wait(barrier, 3)

    gate_sends = [remote(gate_ref.at[pl.ds(pl.multiple_of(relations[r] * count, count), count)], gg.at[r], gs.at[r], gr.at[r], r)
                  for r in range(3)]
    pair_send = remote(u_ref, ug.at[0], us.at[0], ur.at[0], 0)

    def far_send(idx):
        part = pl.ds(pl.multiple_of(idx * piece, piece), piece)
        return remote(u_ref.at[part], ug.at[1, part], us.at[1 + idx], ur.at[1 + idx], 1)

    def relay_send(idx):
        part = pl.ds(pl.multiple_of(idx * piece, piece), piece)
        return remote(ug.at[1, part], ug.at[2, part], us.at[1 + u_chunks + idx], ur.at[1 + u_chunks + idx], 0)

    pair_send.start()
    for send in gate_sends:
        send.start()
    for idx in range(u_chunks):
        far_send(idx).start()

    slots = lax.broadcasted_iota(jnp.int32, (cap, seq), 0)
    lanes = lax.broadcasted_iota(jnp.int32, (cap, 128), 1)

    def finish(row, slot, both):
        act[row, :, slot * col:(slot + 1) * col] = (jax.nn.silu(both[:, :col]) * both[:, col:]).astype(BF16)

    def up_step(phase, index):
        first_expert = 2 * index
        first_tile = (phase * count + first_expert) * wslots
        if phase == 0:
            sources = ((u_ref, gate_ref, me * count), (ug.at[0], gg.at[0], 0))
        else:
            sources = ((ug.at[1], gg.at[1], 0), (ug.at[2], gg.at[2], 0))

        def gather():
            for src, (tokens_ref, gates_ref, offset) in enumerate(sources):
                part = slice(src * cap, (src + 1) * cap)
                picks = []
                for idx in range(2):
                    hit = pos_ref[2 * phase + src, pl.ds(first_expert + idx, 1), :] == slots
                    picks.append(hit.astype(F32).astype(BF16))
                    gate_row = gates_ref[pl.ds(offset + first_expert + idx, 1), :]
                    column = jnp.sum(jnp.where(hit, gate_row, 0.0), axis=-1, keepdims=True)
                    gcol[phase, part, :] = jnp.where(lanes == first_expert + idx, column, gcol[phase, part, :])
                picked = jnp.dot(jnp.concatenate(picks, axis=0), tokens_ref[...], preferred_element_type=F32).astype(BF16)
                rows[0, part, :] = picked[:cap]
                rows[1, part, :] = picked[cap:]

        for start in range(0, 2 * wslots, 2):
            for tile in (start, start + 1):
                for copy in w13_copies(first_tile + tile):
                    copy.wait()
            if start == 0:
                gather()
            row = phase * count + first_expert
            idx, slot = divmod(start, wslots)
            lead = jnp.dot(rows[idx], pool[lax.rem(first_tile + start, ring)], preferred_element_type=F32)
            last_idx, last_slot = divmod(start - 1, wslots)
            finish(lax.rem(row + last_idx + 2 * count, 2 * count), last_slot, raw[...])
            trail = jnp.dot(rows[idx], pool[lax.rem(first_tile + start + 1, ring)], preferred_element_type=F32)
            finish(row + idx, slot, lead)
            raw[...] = trail
            for tile in (start, start + 1):
                ahead = first_tile + tile + ring
                if phase == 0:
                    w13_start(ahead)
                else:
                    @pl.when(ahead < up_tiles)
                    def _(ahead=ahead):
                        w13_start(ahead)

                    @pl.when(ahead >= up_tiles)
                    def _(ahead=ahead):
                        w2_start(ahead - up_tiles)

    gcol[...] = jnp.zeros_like(gcol)
    raw[...] = jnp.zeros_like(raw)
    gate_sends[0].wait_recv()
    pair_send.wait_recv()
    stride = count // 2 // u_chunks

    def near(index, carry):
        up_step(0, index)

        @pl.when(lax.rem(index, stride) == stride - 1)
        def _():
            far_send(index // stride).wait_recv()
            relay_send(index // stride).start()
        return carry
    lax.fori_loop(0, count // 2, near, 0)
    for idx in range(2):
        oh_copy(idx).start()
    gate_sends[1].wait_recv()
    gate_sends[2].wait_recv()
    for idx in range(u_chunks):
        relay_send(idx).wait_recv()

    def away(index, carry):
        up_step(1, index)
        return carry
    lax.fori_loop(0, count // 2, away, 0)
    finish(2 * count - 1, wslots - 1, raw[...])

    total_steps = 2 * chunks * groups

    def pair_sum(order):
        slot = lax.rem(order, 2)
        return remote(acc.at[slot, 1], pair_buf.at[slot], ps.at[slot], pr.at[slot], 0)

    def far_sum(chunk):
        return remote(far_src.at[lax.rem(chunk, 3)], far_dst.at[chunk], xs.at[lax.rem(chunk, 3)], xr.at[chunk], 1)

    def mix(step, order, part):
        slot = lax.rem(step, 3)
        for src in range(2):
            hits = jnp.concatenate([oht[slot, src]] * 3, axis=1)
            mixed = jnp.dot(hits, pst[part % 2, src], preferred_element_type=F32)
            if part == 0:
                acc[lax.rem(order, 2), src] = mixed
            else:
                acc[lax.rem(order, 2), src] += mixed

    def settle(order):
        pair_sum(order).wait_recv()
        pair_sum(order).wait_send()
        slot = lax.rem(order, 2)

        @pl.when(order < chunks)
        def _():
            @pl.when(order == 3)
            def _():
                far_sum(0).wait_send()
            far_src[lax.rem(order, 3)] = acc[slot, 0] + pair_buf[slot]
            far_sum(order).start()

        @pl.when(order >= chunks)
        def _():
            chunk = order - chunks
            far_sum(chunk).wait_recv()
            cols = pl.ds(pl.multiple_of(chunk * block, block), block)
            total = acc[slot, 0] + pair_buf[slot]
            out_ref[:, cols] = (hid_ref[:, cols].astype(F32) + total + far_dst[chunk]).astype(BF16)

    def down(order, carry):
        phase = 1 - order // chunks
        for part in range(groups):
            step = order * groups + part
            slot = lax.rem(step + up_tiles, ring)
            for copy in w2_copies(step):
                copy.wait()
            oh_copy(step).wait()
            for idx in range(per):
                expert = part * per + idx
                done = jnp.dot(act[phase * count + expert], pool[slot, idx * width:(idx + 1) * width, :], preferred_element_type=F32).astype(BF16)
                rest = done.astype(F32) * gcol[phase, :, expert:expert + 1]
                for term in range(3):
                    head = rest.astype(BF16)
                    at = (term * per + idx) * cap
                    pst[part % 2, 0, at:at + cap, :] = head[:cap]
                    pst[part % 2, 1, at:at + cap, :] = head[cap:]
                    rest = rest - head.astype(F32)
            if part > 0:
                mix(step - 1, order, part - 1)
            else:
                @pl.when(order > 0)
                def _():
                    mix(step - 1, order - 1, groups - 1)
                    pair_sum(order - 1).start()

            @pl.when(step + ring < total_steps)
            def _():
                w2_start(step + ring)

            @pl.when(step + 2 < total_steps)
            def _():
                oh_copy(step + 2).start()

            if part == 2:
                @pl.when(order > 0)
                def _():
                    settle(order - 1)
        return carry
    lax.fori_loop(0, 2 * chunks, down, 0)
    last = 2 * chunks - 1
    mix(total_steps - 1, last, groups - 1)
    pair_sum(last).start()
    settle(last)

    for send in gate_sends:
        send.wait_send()
    pair_send.wait_send()
    for idx in range(u_chunks):
        far_send(idx).wait_send()
        relay_send(idx).wait_send()
    for idx in range(1, chunks):
        far_sum(idx).wait_send()


def moe(pos_lane, u_own, gates_lane, hidden, w_one, w_three, w_two, onehot, cap):
    seq, model = u_own.shape
    count, _, width = w_one.shape
    u_chunks, chunks, groups, wslots = 4, 4, 8, 4
    block, per = model // chunks, count // groups
    vmem = pl.BlockSpec(memory_space=pltpu.VMEM)
    hbm = pl.BlockSpec(memory_space=pl.ANY)
    dma = pltpu.SemaphoreType.DMA
    return pl.pallas_call(
        functools.partial(moe_kernel, cap=cap, u_chunks=u_chunks, chunks=chunks, groups=groups, wslots=wslots),
        in_specs=[vmem, vmem, vmem, vmem, hbm, hbm, hbm, hbm],
        out_specs=vmem,
        out_shape=jax.ShapeDtypeStruct((seq, model), BF16),
        scratch_shapes=[
            pltpu.VMEM((3, seq, model), BF16), pltpu.VMEM((3, count, seq), F32), pltpu.VMEM((2, 2 * cap, model), BF16), pltpu.VMEM((2 * cap, block), F32),
            pltpu.VMEM((2 * count, 2 * cap, width), BF16), pltpu.VMEM((2, 2 * cap, 128), F32),
            pltpu.VMEM((6, model, block), BF16),
            pltpu.VMEM((3, 2, seq, per * cap), BF16), pltpu.VMEM((2, 2, 3 * per * cap, block), BF16),
            pltpu.VMEM((2, 2, seq, block), F32), pltpu.VMEM((2, seq, block), F32),
            pltpu.VMEM((3, seq, block), F32), pltpu.VMEM((chunks, seq, block), F32),
            dma((1 + 2 * u_chunks,)), dma((1 + 2 * u_chunks,)), dma((3,)), dma((3,)), dma((6, 2)), dma((3,)),
            dma((2,)), dma((2,)), dma((3,)), dma((chunks,))],
        compiler_params=pltpu.CompilerParams(collective_id=1, has_side_effects=True, vmem_limit_bytes=67043328),
        name='moe',
    )(pos_lane, u_own, gates_lane, hidden, w_one, w_three, w_two, onehot)


def solution(mesh):
    tok_spec = P(('dp', 'ep'))
    row_spec = P('ep')

    def local_layer(tokens, w_query, w_key, w_value, w_out, w_router, w_one, w_three, w_two, expert_ids):
        seq, model = tokens.shape[1:]
        head_dim = w_query.shape[2]
        choices = expert_ids.shape[2]
        experts = w_router.shape[1]
        own_experts = w_one.shape[0]
        cap = 2 * seq * choices // experts
        ids = expert_ids[0]
        flat = [w.reshape(w.shape[0], -1) for w in (w_query, w_key, w_value)]
        hidden, u_own, pos, gates, onehot = front(ids.T, tokens[0], w_router.T, *flat, w_out, cap, own_experts, head_dim)
        return moe(pos, u_own, gates, hidden, w_one, w_three, w_two, onehot, cap)[None]

    return jax.shard_map(local_layer, mesh=mesh, in_specs=(tok_spec, row_spec, row_spec, row_spec, row_spec, P(), row_spec, row_spec, row_spec, tok_spec), out_specs=tok_spec, check_vma=False)
```
